32 devices in a mesh: lat: 4 (over x, core), lon: 8 (over z, y).
Axes of the slice: x: 2, y: 2, z: 4, core: 2. Of those that a mesh axis runs over, the one named last changes fastest.
Arguments:
- node_latent: bfloat16 [64, 256, 512], P('lat', 'lon'), may hold values from -6 to 6
- edge_latent: bfloat16 [65536, 512], P(('lat', 'lon')), may hold values from -6 to 6
- sender: int32 [65536], P(('lat', 'lon')), may hold values from -1 to 16383, as said below
- receiver: int32 [65536], P(('lat', 'lon')), may hold values from -1 to 127, as said below
- block_tile: int32 [512], P(('lat', 'lon')), may hold values from 0 to 3, as said below
- w_first: bfloat16 [1536, 512], replicated, may hold values from -0.15625 to 0.15625
- w_second: bfloat16 [512, 512], replicated, may hold values from -0.25 to 0.25
- edge_gain: float32 [512], replicated, may hold values from 0.5 to 1.5
- w_node_first: bfloat16 [1024, 512], replicated, may hold values from -0.1875 to 0.1875
- w_node_second: bfloat16 [512, 512], replicated, may hold values from -0.25 to 0.25
- node_gain: float32 [512], replicated, may hold values from 0.5 to 1.5
Outputs:
- node_out: bfloat16 [64, 256, 512], P('lat', 'lon')
- edge_out: bfloat16 [65536, 512], P(('lat', 'lon'))
The draws below stay inside these ranges and needn't reach their ends.
Inputs may be any that keep to these rules, and one draw needn't show every extreme that they name: `sender`: -1 on padded slots; otherwise the id of one of the eight grid neighbours of the edge's receiver node (columns wrap around, rows do not), or of a node whose row and column are both multiples of 4, anywhere on the grid. `receiver`: padded slots (-1) stand at the end of each block, at least 32 slots of a block are live, and live values never fall within a block. `block_tile`: never falls from one block of a device to the next, over the device's 16 blocks.
All inputs are finite; a program needn't handle non-finite values.
Results may differ from the reference program's by a relative error of at most 0.008.
Values may be sent and summed in bfloat16 or wider, within the bound.
A program may use at most 128 MiB of HBM per device.

```python
import jax
import jax.numpy as jnp
import numpy as np
from jax import lax

D = 512
PR = 16
PC = 32
BLOCKS_DEV = 16
BLK = 128
TILE_NODES = 128
NODE_DEV = 512
EDGE_DEV = 2048
NLAT = 64
NLON = 256
NODES = 16384
EDGES = 65536
N_LAT = 4
N_LON = 8
DEVICES = 32


def edge_plan(key):
    folded = jax.random.fold_in(key, 1013)
    subkeys = jax.random.split(folded, 7)
    grid_rows = PR * N_LAT
    grid_cols = PC * N_LON
    tile_count = PR // 4
    shape = (DEVICES, BLOCKS_DEV, BLK)
    device = jnp.arange(DEVICES, dtype=jnp.int32)[:, None]
    block_pos = jnp.arange(BLOCKS_DEV, dtype=jnp.int32)[None, :]
    offset = jax.random.randint(subkeys[0], (DEVICES, 1), -1, 2)
    tile_of = jnp.clip((block_pos + offset) * tile_count // BLOCKS_DEV, 0, tile_count - 1).astype(jnp.int32)
    live_count = jax.random.randint(subkeys[1], (DEVICES, BLOCKS_DEV, 1), BLK // 4, BLK + 1)
    slot_pos = jnp.arange(BLK, dtype=jnp.int32)[None, None, :]
    live_slot = slot_pos < live_count
    within = jnp.sort(jax.random.randint(subkeys[2], shape, 0, 4 * PC), axis=2)
    receiver = jnp.where(live_slot, within, -1)
    local_index = tile_of[:, :, None] * (4 * PC) + within
    lat_band = (device // N_LON)[:, :, None]
    lon_sector = (device % N_LON)[:, :, None]
    recv_row = lat_band * PR + local_index // PC
    recv_col = lon_sector * PC + local_index % PC
    picked = jax.random.randint(subkeys[3], shape, 0, 8)
    row_table = jnp.array(np.array([-1, -1, -1, 0, 0, 1, 1, 1], np.int32))
    col_table = jnp.array(np.array([-1, 0, 1, -1, 1, -1, 0, 1], np.int32))
    step_row = row_table[picked]
    step_col = col_table[picked]
    near_row = recv_row + step_row
    near_row = jnp.where((near_row < 0) | (near_row >= grid_rows), recv_row - step_row, near_row)
    near_col = (recv_col + step_col) % grid_cols
    is_polar = (lat_band == 0) | (lat_band == N_LAT - 1)
    coin_flip = jax.random.randint(subkeys[4], shape, 0, 4)
    is_far = coin_flip < jnp.where(is_polar, 2, 1)
    coarse_row = 4 * jax.random.randint(subkeys[5], shape, 0, grid_rows // 4)
    coarse_col = 4 * jax.random.randint(subkeys[6], shape, 0, grid_cols // 4)
    sender = jnp.where(is_far, coarse_row * grid_cols + coarse_col, near_row * grid_cols + near_col)
    sender = jnp.where(live_slot, sender, -1)
    return (sender.reshape(-1).astype(jnp.int32), receiver.reshape(-1).astype(jnp.int32), tile_of.reshape(-1))


def draw_sender(key, part):
    return edge_plan(key)[0]


def draw_receiver(key, part):
    return edge_plan(key)[1]


def draw_block_tile(key, part):
    return edge_plan(key)[2]


def shard_levels(stream_key, extent, shards, low, high):
    loudness, own = 1.0, jax.random.fold_in(stream_key, 6)
    for dim, blocks in shards:
        steps = jnp.exp(jax.random.uniform(jax.random.fold_in(own, dim), (blocks,), jnp.float32, low / len(shards), high / len(shards)))
        loudness = loudness * jnp.repeat(steps, extent[dim] // blocks).reshape([-1 if axis == dim else 1 for axis in range(len(extent))])
    return loudness


def noise(own_key, dims, scale, reach, shards=(), held_as=jnp.bfloat16):
    values = jax.random.normal(own_key, dims, jnp.float32) * scale
    if len(shards) > 0:
        values = shard_levels(own_key, dims, shards, -0.22, 0.18) * values
    return jnp.clip(values, min=-reach, max=reach).astype(held_as)


def setup_inputs(seed: int = 0) -> dict:
    keys = jax.random.split(jax.random.key(seed), 12)
    return {
        "node_latent": noise(keys[0], (NLAT, NLON, D), 1.0, 6.0, ((0, 4), (1, 8))),
        "edge_latent": noise(keys[1], (EDGES, D), 1.0, 6.0, ((0, 32),)),
        "sender": draw_sender(jax.random.fold_in(keys[11], 71), 0),
        "receiver": draw_receiver(jax.random.fold_in(keys[11], 71), 0),
        "block_tile": draw_block_tile(jax.random.fold_in(keys[11], 71), 0),
        "w_first": noise(keys[5], (3 * D, D), (3 * D) ** -0.5, 0.15625),
        "w_second": noise(keys[6], (D, D), D ** -0.5, 0.25),
        "edge_gain": jnp.clip(1.0 + 0.1 * jax.random.normal(keys[7], (D,), jnp.float32), 0.5, 1.5),
        "w_node_first": noise(keys[8], (2 * D, D), (2 * D) ** -0.5, 0.1875),
        "w_node_second": noise(keys[9], (D, D), D ** -0.5, 0.25),
        "node_gain": jnp.clip(1.0 + 0.1 * jax.random.normal(keys[10], (D,), jnp.float32), 0.5, 1.5),
    }


def layer_norm(values, gain_vec):
    average = lax.optimization_barrier(jnp.mean(values, -1, keepdims=True))
    centred = values - average
    spread = lax.optimization_barrier(jnp.mean(centred * centred, -1, keepdims=True))
    return centred * lax.rsqrt(spread + 1e-05) * gain_vec

def reference(node_latent, edge_latent, sender, receiver, block_tile, w_first, w_second, edge_gain, w_node_first, w_node_second, node_gain):
    node_rows = node_latent.reshape(NODES, D)
    edge_parts = edge_latent.reshape(DEVICES, EDGE_DEV, D)
    send_parts = sender.reshape(DEVICES, EDGE_DEV)
    recv_parts = receiver.reshape(DEVICES, EDGE_DEV)
    tile_parts = jnp.broadcast_to(block_tile.reshape(DEVICES, BLOCKS_DEV, 1), (DEVICES, BLOCKS_DEV, BLK)).reshape(DEVICES, EDGE_DEV)

    def one_device(pieces):
        edge_rows, senders, receivers, tile_of, device = pieces
        live_slot = receivers >= 0
        local_index = tile_of * TILE_NODES + jnp.maximum(receivers, 0)
        lat_band = device // N_LON
        lon_sector = device % N_LON
        recv_row = lat_band * PR + local_index // PC
        recv_col = lon_sector * PC + local_index % PC
        recv_rows = node_rows[recv_row * NLON + recv_col]
        send_rows = node_rows[jnp.maximum(senders, 0)]
        joined = jnp.concatenate([edge_rows, send_rows, recv_rows], axis=1)
        first_sum = jnp.dot(joined, w_first, preferred_element_type=jnp.float32)
        hidden = jax.nn.silu(first_sum).astype(jnp.bfloat16)
        second_sum = jnp.dot(hidden, w_second, preferred_element_type=jnp.float32)
        message = layer_norm(second_sum, edge_gain).astype(jnp.bfloat16)
        updated = jnp.where(live_slot[:, None], edge_rows.astype(jnp.float32) + message.astype(jnp.float32), jnp.zeros((), jnp.float32)).astype(jnp.bfloat16)
        segment = jnp.where(live_slot, local_index, NODE_DEV).astype(jnp.int32)
        summed = jax.ops.segment_sum(message.astype(jnp.float32), segment, num_segments=NODE_DEV + 1)[:NODE_DEV]
        return (updated, summed)
    device_ids = jnp.arange(DEVICES, dtype=jnp.int32)
    updated, summed = lax.map(one_device, (edge_parts, send_parts, recv_parts, tile_parts, device_ids))
    aggregate = summed.reshape(N_LAT, N_LON, PR, PC, D).transpose(0, 2, 1, 3, 4).reshape(NODES, D).astype(jnp.bfloat16)
    node_join = jnp.concatenate([node_rows, aggregate], axis=1)
    node_hidden = jax.nn.silu(jnp.dot(node_join, w_node_first, preferred_element_type=jnp.float32)).astype(jnp.bfloat16)
    node_second = jnp.dot(node_hidden, w_node_second, preferred_element_type=jnp.float32)
    node_out = (node_rows.astype(jnp.float32) + layer_norm(node_second, node_gain)).astype(jnp.bfloat16)
    return (node_out.reshape(NLAT, NLON, D), updated.reshape(EDGES, D))
```

```python
import functools

import jax
import jax.numpy as jnp
from jax import lax
from jax.experimental import pallas as pl
from jax.experimental.pallas import tpu as pltpu
from jax.sharding import PartitionSpec as P

F32 = jnp.float32
BF16 = jnp.bfloat16
LANES = 128
CHUNK = 32
MIB = 1024 * 1024


def dot(a, b):
    return jnp.dot(a, b, preferred_element_type=F32)


def silu(value):
    half = 0.5 * value
    return half * (1.0 + jnp.tanh(half))


def layer_norm(values, gain_vec):
    average = jnp.mean(values, -1, keepdims=True)
    centred = values - average
    spread = jnp.mean(centred * centred, -1, keepdims=True)
    return centred * lax.rsqrt(spread + 1e-05) * gain_vec


def power_of_two(n):
    return n & (n - 1) == 0


def quotient(value, n):
    if power_of_two(n):
        return lax.shift_right_arithmetic(value, jnp.full_like(value, n.bit_length() - 1))
    return lax.div(value, jnp.full_like(value, n))


def remainder(value, n):
    if power_of_two(n):
        return value & (n - 1)
    return lax.rem(value, jnp.full_like(value, n))


def plan(patch_rows, patch_cols, lat_count, lon_count):
    cores = 2 if lat_count % 2 == 0 else 1
    low = 1
    while lon_count % (4 * low) == 0 and 4 * low * low <= lon_count:
        low *= 2
    left = patch_rows * patch_cols
    right = left + patch_rows
    top = right + patch_rows
    bottom = top + patch_cols
    corners = bottom + patch_cols
    coarse_at = corners + 32
    per = patch_rows // 4 * (patch_cols // 4)
    return dict(
        cores=cores,
        wide=lat_count // cores,
        high=lon_count // low,
        low=low,
        near=(left, right, top, bottom, corners, coarse_at),
        per=per,
        length=coarse_at + per * lat_count * lon_count,
    )


def sender_rows(sender, lat, lon, patch_rows, patch_cols, lon_count, shape):
    grid_cols = patch_cols * lon_count
    left, right, top, bottom, corners, coarse_at = shape["near"]
    send_row, send_col = quotient(sender, grid_cols), remainder(sender, grid_cols)
    row = send_row - lat * patch_rows
    col = remainder(send_col - lon * patch_cols + 1 + grid_cols, grid_cols) - 1
    is_near = (row >= -1) & (row <= patch_rows) & (col <= patch_cols)
    inside = (col >= 0) & (col < patch_cols)
    side = jnp.where(col < 0, left, right)
    corner = corners + jnp.where(col < 0, 0, 16)
    top_index = jnp.where(inside, top + col, corner + 7)
    bottom_index = jnp.where(inside, bottom + col, corner + 8)
    middle = jnp.where(inside, row * patch_cols + col, side + row)
    near_index = jnp.where(row < 0, top_index, jnp.where(row >= patch_rows, bottom_index, middle))
    at_lat, at_lon = quotient(send_row, patch_rows), quotient(send_col, patch_cols)
    core, across = remainder(at_lat, shape["cores"]), quotient(at_lat, shape["cores"])
    high, low = quotient(at_lon, shape["low"]), remainder(at_lon, shape["low"])
    block = ((high * shape["cores"] + core) * shape["wide"] + across) * shape["low"] + low
    far_index = (
        coarse_at
        + block * shape["per"]
        + quotient(remainder(send_row, patch_rows), 4) * (patch_cols // 4)
        + quotient(remainder(send_col, patch_cols), 4)
    )
    return jnp.where(sender < 0, 0, jnp.where(is_near, near_index, far_index))


def border_hot(patch_rows, patch_cols, first_row, rows):
    count = patch_rows * patch_cols
    coarse_cols = patch_cols // 4
    coarse = patch_rows // 4 * coarse_cols
    pick = lax.broadcasted_iota(jnp.int32, (rows, count), 0) + first_row
    node = lax.broadcasted_iota(jnp.int32, (rows, count), 1)
    from_coarse = quotient(pick, coarse_cols) * (4 * patch_cols) + remainder(pick, coarse_cols) * 4
    side = pick - coarse
    from_side = jnp.where(
        side < patch_rows, side * patch_cols, (side - patch_rows) * patch_cols + patch_cols - 1
    )
    return jnp.where(node == jnp.where(pick < coarse, from_coarse, from_side), 1.0, 0.0).astype(BF16)


def gather_kernel(
    shape,
    patch_rows,
    patch_cols,
    tile_nodes,
    node_hbm,
    edge_hbm,
    send_hbm,
    recv_hbm,
    tile_hbm,
    w_hbm,
    first_ref,
    sent_ref,
    index_ref,
    own_ref,
    edge_ref,
    send_ref,
    recv_ref,
    tile_ref,
    w_ref,
    side_ref,
    table_ref,
    received_ref,
    load_sem,
    edge_sem,
    halo_send,
    halo_recv,
    line_send,
    line_recv,
    plane_send,
    plane_recv,
    core_send,
    core_recv,
):
    lat_count, lon_count = lax.axis_size("lat"), lax.axis_size("lon")
    lat, lon = lax.axis_index("lat"), lax.axis_index("lon")
    cores, wide, high_count, low_count = (shape[k] for k in ("cores", "wide", "high", "low"))
    per = shape["per"]
    node_count, features = own_ref.shape
    left, right, top, bottom, corners, coarse_at = (at - node_count for at in shape["near"])
    core, across = lax.rem(lat, cores), lax.div(lat, cores)
    high, low = lax.div(lon, low_count), lax.rem(lon, low_count)
    tiles = features // LANES
    blocks, block_len = recv_ref.shape

    def load(source, target, i):
        return pltpu.make_async_copy(source, target, load_sem.at[i])

    loads = [
        load(node_hbm, own_ref, 0),
        load(w_hbm, w_ref, 1),
        load(send_hbm, send_ref, 2),
        load(recv_hbm, recv_ref, 3),
        load(tile_hbm, tile_ref, 4),
    ]
    edge_load = pltpu.make_async_copy(edge_hbm, edge_ref, edge_sem)
    loads[0].start()

    def device(at_across, at_core, at_high, at_low):
        return at_across * cores + at_core, at_high * low_count + at_low

    offsets = [(a, b) for a in range(wide) for b in range(low_count)][1:]

    def turn(at, step, count):
        return lax.rem(at + step, count) if step else at

    def line_to(k):
        return device(across, core, turn(high, k, high_count), low)

    def plane_to(step):
        return device(turn(across, step[0], wide), core, high, turn(low, step[1], low_count))

    partner = device(across, 1 - core, high, low)

    last = patch_rows
    halos = (
        (side_ref, last, patch_rows, left, 0, 1),
        (side_ref, 0, patch_rows, right, 0, -1),
        (own_ref, node_count - patch_cols, patch_cols, top, 1, 0),
        (own_ref, 0, patch_cols, bottom, -1, 0),
        (side_ref, last + patch_rows - 8, 8, corners, 1, 1),
        (side_ref, last, 8, corners + 8, -1, 1),
        (side_ref, patch_rows - 8, 8, corners + 16, 1, -1),
        (side_ref, 0, 8, corners + 24, -1, -1),
    )

    def halo_to(i):
        return (
            lax.rem(lat + halos[i][4] + lat_count, lat_count),
            lax.rem(lon + halos[i][5] + lon_count, lon_count),
        )

    barrier = pltpu.get_barrier_semaphore()
    greeted = [line_to(k) for k in range(1, high_count)] + [plane_to(step) for step in offsets]
    greeted += [partner] if cores == 2 else []
    greeted += [halo_to(i) for i in range(len(halos))]
    for at in greeted:
        pl.semaphore_signal(
            barrier, inc=1, device_id=at, device_id_type=pl.DeviceIdType.MESH
        )
    for each in loads[1:]:
        each.start()
    edge_load.start()

    def slots(at_high, at_core, at_across, at_low, count=1):
        block = ((at_high * cores + at_core) * wide + at_across) * low_count + at_low
        return pl.ds(pl.multiple_of(coarse_at + block * per, 8), count * per)

    def copy(source, target, send_sem, recv_sem, at):
        return pltpu.make_async_remote_copy(
            src_ref=source,
            dst_ref=target,
            send_sem=send_sem,
            recv_sem=recv_sem,
            device_id=at,
            device_id_type=pl.DeviceIdType.MESH,
        )

    def line(k, origin):
        block = table_ref.at[slots(origin, core, across, low), :]
        return copy(block, block, line_send.at[k], line_recv.at[k], line_to(k))

    def line_out(k):
        return line(k, high)

    def line_in(k):
        return line(k, turn(high, high_count - k, high_count))

    def from_high(j):
        return turn(high, (high_count - j) % high_count, high_count)

    def plane(j, i, at_across, at_low):
        block = table_ref.at[slots(from_high(j), core, at_across, at_low), :]
        return copy(block, block, plane_send.at[j, i], plane_recv.at[j, i], plane_to(offsets[i]))

    def plane_out(j, i):
        return plane(j, i, across, low)

    def plane_in(j, i):
        a, b = offsets[i]
        return plane(
            j,
            i,
            turn(across, (wide - a) % wide, wide),
            turn(low, (low_count - b) % low_count, low_count),
        )

    def pair(j, at_core):
        block = table_ref.at[slots(from_high(j), at_core, 0, 0, wide * low_count), :]
        return copy(block, block, core_send.at[j], core_recv.at[j], partner)

    def halo(i):
        ref, start, size, target, _, _ = halos[i]
        return copy(
            ref.at[start : start + size, :],
            table_ref.at[target : target + size, :],
            halo_send.at[i],
            halo_recv.at[i],
            halo_to(i),
        )

    def sends(i):
        there = lat + halos[i][4]
        return (there >= 0) & (there < lat_count)

    def receives(i):
        origin = lat - halos[i][4]
        return (origin >= 0) & (origin < lat_count)

    coarse_hot = border_hot(patch_rows, patch_cols, 0, per)
    side_hot = border_hot(patch_rows, patch_cols, per, 2 * patch_rows)
    loads[0].wait()
    own = own_ref[...]
    table_ref[slots(high, core, across, low), :] = dot(coarse_hot, own).astype(BF16)
    side_ref[...] = dot(side_hot, own).astype(BF16)
    for i, (_, _, size, target, _, _) in enumerate(halos):

        @pl.when(jnp.logical_not(receives(i)))
        def _():
            table_ref[target : target + size, :] = jnp.zeros((size, features), BF16)

    pl.semaphore_wait(barrier, len(greeted))
    for k in range(1, high_count):
        line_out(k).start()
    for i in range(len(offsets)):
        plane_out(0, i).start()
    for i in range(len(halos)):
        pl.when(sends(i))(lambda i=i: halo(i).start())

    def relay_line(k):
        line_in(k).wait_recv()
        for i in range(len(offsets)):
            plane_out(k, i).start()

    def relay_plane(j):
        for i in range(len(offsets)):
            plane_in(j, i).wait_recv()
        if cores == 2:
            pair(j, core).start()

    def project(rows, start):
        result = dot(rows, w_ref[features : 2 * features, :])
        for t in range(tiles):
            sent_ref[pl.ds(start * tiles + t, rows.shape[0], stride=tiles), :] = result[
                :, t * LANES : (t + 1) * LANES
            ]

    def project_coarse(j):
        if cores == 2:
            pair(j, 1 - core).wait_recv()
        count = cores * wide * low_count * per
        rows = slots(from_high(j), 0, 0, 0, cores * wide * low_count)
        start = pl.multiple_of(node_count + coarse_at + from_high(j) * count, 8)
        project(table_ref[rows, :], start)

    def first_layer(g, size):
        rows = slice(g * size, (g + 1) * size)
        received = []
        for i in range(g * size // block_len, (g + 1) * size // block_len):
            local = recv_ref[i : i + 1, :] + tile_ref[i] * tile_nodes
            spread = jnp.broadcast_to(local, (LANES, block_len)).T
            lane = lax.broadcasted_iota(jnp.int32, (block_len, LANES), 1)
            parts = [
                jnp.where(spread == lane + at, 1.0, 0.0).astype(BF16)
                for at in range(0, node_count, LANES)
            ]
            received.append(jnp.concatenate(parts, axis=1))
        first_ref[rows, :] = dot(edge_ref[rows, :], w_ref[:features, :]) + dot(
            jnp.concatenate(received, axis=0), received_ref[...]
        )

    loads[2].wait()
    index_ref[...] = tiles * sender_rows(
        send_ref[...], lat, lon, patch_rows, patch_cols, lon_count, shape
    )
    loads[1].wait()
    received_ref[...] = dot(own, w_ref[2 * features :, :]).astype(BF16)
    project(own, 0)
    loads[3].wait()
    loads[4].wait()
    edge_load.wait()

    groups = 8 if blocks % 8 == 0 else 1
    size = blocks * block_len // groups
    work = [functools.partial(first_layer, g, size) for g in range(groups)]

    def do(count):
        for _ in range(min(count, len(work))):
            work.pop(0)()

    for k in range(1, high_count):
        relay_line(k)
        do(1)
    relay_plane(0)
    do(2)
    for j in range(1, high_count):
        relay_plane(j)
        do(1)
        if j == 1:
            do(len(work))
            for i in range(len(halos)):
                pl.when(receives(i))(lambda i=i: halo(i).wait_recv())
            project(table_ref[:coarse_at, :], node_count)
        project_coarse(j - 1)
    do(len(work))
    project_coarse(high_count - 1)

    for k in range(1, high_count):
        line_out(k).wait_send()
    for j in range(high_count):
        for i in range(len(offsets)):
            plane_out(j, i).wait_send()
        if cores == 2:
            pair(j, core).wait_send()
    for i in range(len(halos)):
        pl.when(sends(i))(lambda i=i: halo(i).wait_send())


def in_hbm(*arrays):
    return [pltpu.with_memory_space_constraint(each, pltpu.HBM) for each in arrays]


def gather(shape, node, edges, senders, receivers, block_tile, w_first, patch_rows, patch_cols):
    node_count, features = node.shape
    edge_count = edges.shape[0]
    blocks, block_len = receivers.shape
    tiles = features // LANES
    near = shape["near"][-1] - node_count
    high = shape["high"]
    others = max(shape["wide"] * shape["low"] - 1, 1)
    dma = pltpu.SemaphoreType.DMA
    hbm, vmem = pl.BlockSpec(memory_space=pltpu.HBM), pl.BlockSpec(memory_space=pltpu.VMEM)
    return pl.pallas_call(
        functools.partial(gather_kernel, shape, patch_rows, patch_cols, 4 * patch_cols),
        in_specs=[hbm] * 6,
        out_specs=[vmem] * 3,
        out_shape=[
            pltpu.VMEM((edge_count, features), F32),
            pltpu.VMEM((shape["length"] * tiles, LANES), F32),
            pltpu.VMEM((blocks, block_len), jnp.int32),
        ],
        scratch_shapes=[
            pltpu.VMEM((node_count, features), BF16),
            pltpu.VMEM((edge_count, features), BF16),
            pltpu.VMEM((blocks, block_len), jnp.int32),
            pltpu.VMEM((blocks, block_len), jnp.int32),
            pltpu.SMEM((blocks,), jnp.int32),
            pltpu.VMEM(w_first.shape, BF16),
            pltpu.VMEM((2 * patch_rows, features), BF16),
            pltpu.VMEM((shape["length"] - node_count, features), BF16),
            pltpu.VMEM((node_count, features), BF16),
            dma((5,)),
            dma,
            dma((8,)),
            dma((8,)),
            dma((high,)),
            dma((high,)),
            dma((high, others)),
            dma((high, others)),
            dma((high,)),
            dma((high,)),
        ],
        compiler_params=pltpu.CompilerParams(
            has_side_effects=True, collective_id=0, vmem_limit_bytes=20 * MIB
        ),
        cost_estimate=pl.CostEstimate(
            flops=8 * edge_count * features * features, bytes_accessed=8 * MIB, transcendentals=0
        ),
    )(*in_hbm(node, edges, senders, receivers, block_tile, w_first))


def update_kernel(
    group,
    tile_nodes,
    index_ref,
    first_ref,
    sent_ref,
    tile_hbm,
    edge_hbm,
    recv_hbm,
    node_hbm,
    w_second_hbm,
    edge_gain_hbm,
    w_node_first_hbm,
    w_node_second_hbm,
    node_gain_hbm,
    node_out_hbm,
    edge_out_hbm,
    tile_ref,
    edge_ref,
    recv_ref,
    own_ref,
    w_second_ref,
    edge_gain_ref,
    w_node_first_ref,
    w_node_second_ref,
    node_gain_ref,
    picked_ref,
    hidden_ref,
    second_ref,
    message_ref,
    edge_out_ref,
    total_ref,
    node_out_ref,
    load_sem,
    out_sem,
):
    edge_count, features = edge_ref.shape
    tiles = features // LANES
    block_len = recv_ref.shape[1]
    groups = edge_count // group
    pairs = (
        (w_second_hbm, w_second_ref),
        (edge_gain_hbm, edge_gain_ref),
        (edge_hbm, edge_ref),
        (recv_hbm, recv_ref),
        (tile_hbm, tile_ref),
        (node_hbm, own_ref),
        (w_node_first_hbm, w_node_first_ref),
        (w_node_second_hbm, w_node_second_ref),
        (node_gain_hbm, node_gain_ref),
    )
    loads = [
        pltpu.make_async_copy(source, target, load_sem.at[i])
        for i, (source, target) in enumerate(pairs)
    ]
    for each in loads:
        each.start()
    total_ref[...] = jnp.zeros_like(total_ref)

    def pick(g):
        slot = g % 2
        for e in range(group):
            at = g * group + e
            start = pl.multiple_of(index_ref[at // block_len, at % block_len], tiles)
            picked_ref[slot, e * tiles : (e + 1) * tiles, :] = sent_ref[pl.ds(start, tiles), :]

    def hide(g):
        slot = g % 2
        for r in range(0, group, CHUNK):
            at = g * group + r
            parts = []
            for t in range(tiles):
                first = (
                    first_ref[at : at + CHUNK, t * LANES : (t + 1) * LANES]
                    + picked_ref[slot, pl.ds(r * tiles + t, CHUNK, stride=tiles), :]
                )
                parts.append(silu(first).astype(BF16))
            hidden_ref[slot, r : r + CHUNK, :] = jnp.concatenate(parts, axis=1)

    def finish(g):
        slot = g % 2
        for i in range(group // block_len):
            block = g * (group // block_len) + i
            receiver = recv_ref[block : block + 1, :]
            spread = jnp.broadcast_to(receiver, (LANES, block_len)).T
            for r in range(i * block_len, (i + 1) * block_len, CHUNK):
                at = g * group + r
                second = second_ref[slot, r : r + CHUNK, :]
                message = layer_norm(second, edge_gain_ref[...]).astype(BF16)
                message_ref[slot, r : r + CHUNK, :] = message
                updated = edge_ref[at : at + CHUNK, :].astype(F32) + message.astype(F32)
                live = spread[r % block_len : r % block_len + CHUNK, :]
                live = jnp.concatenate([live] * tiles, axis=1)
                edge_out_ref[at : at + CHUNK, :] = jnp.where(live >= 0, updated, 0.0).astype(BF16)
            start = pl.multiple_of(tile_ref[block] * tile_nodes, tile_nodes)
            node = lax.broadcasted_iota(jnp.int32, (tile_nodes, block_len), 0)
            hot = jnp.where(node == receiver, 1.0, 0.0).astype(BF16)
            total_ref[pl.ds(start, tile_nodes), :] += dot(
                hot, message_ref[slot, i * block_len : (i + 1) * block_len, :]
            )

    def store(g):
        rows = pl.ds(g * group, group)
        return pltpu.make_async_copy(
            edge_out_ref.at[rows, :], edge_out_hbm.at[rows, :], out_sem.at[g]
        )

    for g in range(groups):
        pick(g)
        hide(g)
        if g == 0:
            loads[0].wait()
        second_ref[g % 2] = dot(hidden_ref[g % 2], w_second_ref[...])
        if g == 0:
            for each in loads[1:5]:
                each.wait()
        finish(g)
        store(g).start()

    for each in loads[5:]:
        each.wait()
    own = own_ref[...]
    node_first = dot(own, w_node_first_ref[:features, :]) + dot(
        total_ref[...].astype(BF16), w_node_first_ref[features:, :]
    )
    node_second = dot(silu(node_first).astype(BF16), w_node_second_ref[...])
    node_out_ref[...] = (
        own.astype(F32) + layer_norm(node_second, node_gain_ref[...])
    ).astype(BF16)
    node_store = pltpu.make_async_copy(node_out_ref, node_out_hbm, out_sem.at[groups])
    node_store.start()
    for g in range(groups):
        store(g).wait()
    node_store.wait()


def update(index, first, sent, block_tile, edges, receivers, node, weights, tile_nodes):
    edge_count, features = edges.shape
    node_count = node.shape[0]
    blocks, block_len = receivers.shape
    tiles = features // LANES
    group = 4 * block_len if blocks % 4 == 0 else block_len
    groups = edge_count // group
    hbm, vmem = pl.BlockSpec(memory_space=pltpu.HBM), pl.BlockSpec(memory_space=pltpu.VMEM)
    loaded = (edges, receivers, node, *weights)
    return pl.pallas_call(
        functools.partial(update_kernel, group, tile_nodes),
        in_specs=[pl.BlockSpec(memory_space=pltpu.SMEM), vmem, vmem] + [hbm] * 9,
        out_specs=[hbm, hbm],
        out_shape=[
            jax.ShapeDtypeStruct((node_count, features), BF16),
            jax.ShapeDtypeStruct((edge_count, features), BF16),
        ],
        scratch_shapes=[pltpu.SMEM((blocks,), jnp.int32)]
        + [pltpu.VMEM(each.shape, each.dtype) for each in loaded]
        + [
            pltpu.VMEM((2, group * tiles, LANES), F32),
            pltpu.VMEM((2, group, features), BF16),
            pltpu.VMEM((2, group, features), F32),
            pltpu.VMEM((2, group, features), BF16),
            pltpu.VMEM((edge_count, features), BF16),
            pltpu.VMEM((node_count, features), F32),
            pltpu.VMEM((node_count, features), BF16),
            pltpu.SemaphoreType.DMA((9,)),
            pltpu.SemaphoreType.DMA((groups + 1,)),
        ],
        compiler_params=pltpu.CompilerParams(vmem_limit_bytes=24 * MIB),
    )(index, first, sent, *in_hbm(block_tile, *loaded))


def per_device(
    node_latent,
    edge_latent,
    sender,
    receiver,
    block_tile,
    w_first,
    w_second,
    edge_gain,
    w_node_first,
    w_node_second,
    node_gain,
):
    patch_rows, patch_cols, features = node_latent.shape
    blocks = block_tile.shape[0]
    shape = plan(patch_rows, patch_cols, lax.axis_size("lat"), lax.axis_size("lon"))
    node = node_latent.reshape(patch_rows * patch_cols, features)
    receivers = receiver.reshape(blocks, -1)
    first, sent, index = gather(
        shape,
        node,
        edge_latent,
        sender.reshape(blocks, -1),
        receivers,
        block_tile,
        w_first,
        patch_rows,
        patch_cols,
    )
    weights = (
        w_second,
        edge_gain.reshape(1, -1),
        w_node_first,
        w_node_second,
        node_gain.reshape(1, -1),
    )
    node_out, edge_out = update(
        index, first, sent, block_tile, edge_latent, receivers, node, weights, 4 * patch_cols
    )
    return node_out.reshape(patch_rows, patch_cols, features), edge_out


def solution(mesh):
    return jax.shard_map(
        per_device,
        mesh=mesh,
        in_specs=(
            P("lat", "lon", None),
            P(("lat", "lon"), None),
            P(("lat", "lon")),
            P(("lat", "lon")),
            P(("lat", "lon")),
            P(),
            P(),
            P(),
            P(),
            P(),
            P(),
        ),
        out_specs=(P("lat", "lon", None), P(("lat", "lon"), None)),
        check_vma=False,
    )
```

```python
import functools

import jax
import jax.numpy as jnp
from jax import lax
from jax.experimental import pallas as pl
from jax.experimental.pallas import tpu as pltpu
from jax.sharding import PartitionSpec as P

F32 = jnp.float32
BF16 = jnp.bfloat16
LANES = 128
CHUNK = 32
MIB = 1024 * 1024


def dot(a, b):
    return jnp.dot(a, b, preferred_element_type=F32)


def layer_norm(values, gain_vec):
    average = jnp.mean(values, -1, keepdims=True)
    centred = values - average
    spread = jnp.mean(centred * centred, -1, keepdims=True)
    return centred * lax.rsqrt(spread + 1e-05) * gain_vec


def power_of_two(n):
    return n & (n - 1) == 0


def quotient(value, n):
    if power_of_two(n):
        return lax.shift_right_arithmetic(value, jnp.full_like(value, n.bit_length() - 1))
    return lax.div(value, jnp.full_like(value, n))


def remainder(value, n):
    if power_of_two(n):
        return value & (n - 1)
    return lax.rem(value, jnp.full_like(value, n))


def plan(patch_rows, patch_cols, lat_count, lon_count):
    cores = 2 if lat_count % 2 == 0 else 1
    low = 1
    while lon_count % (4 * low) == 0 and 4 * low * low <= lon_count:
        low *= 2
    left = patch_rows * patch_cols
    right = left + patch_rows
    top = right + patch_rows
    bottom = top + patch_cols
    corners = bottom + patch_cols
    coarse_at = corners + 32
    per = patch_rows // 4 * (patch_cols // 4)
    return dict(
        cores=cores,
        wide=lat_count // cores,
        high=lon_count // low,
        low=low,
        near=(left, right, top, bottom, corners, coarse_at),
        per=per,
        length=coarse_at + per * lat_count * lon_count,
    )


def sender_rows(sender, lat, lon, patch_rows, patch_cols, lon_count, shape):
    grid_cols = patch_cols * lon_count
    left, right, top, bottom, corners, coarse_at = shape["near"]
    send_row, send_col = quotient(sender, grid_cols), remainder(sender, grid_cols)
    row = send_row - lat * patch_rows
    col = remainder(send_col - lon * patch_cols + 1 + grid_cols, grid_cols) - 1
    is_near = (row >= -1) & (row <= patch_rows) & (col <= patch_cols)
    inside = (col >= 0) & (col < patch_cols)
    side = jnp.where(col < 0, left, right)
    corner = corners + jnp.where(col < 0, 0, 16)
    top_index = jnp.where(inside, top + col, corner + 7)
    bottom_index = jnp.where(inside, bottom + col, corner + 8)
    middle = jnp.where(inside, row * patch_cols + col, side + row)
    near_index = jnp.where(row < 0, top_index, jnp.where(row >= patch_rows, bottom_index, middle))
    at_lat, at_lon = quotient(send_row, patch_rows), quotient(send_col, patch_cols)
    core, across = remainder(at_lat, shape["cores"]), quotient(at_lat, shape["cores"])
    high, low = quotient(at_lon, shape["low"]), remainder(at_lon, shape["low"])
    block = ((high * shape["cores"] + core) * shape["wide"] + across) * shape["low"] + low
    far_index = (
        coarse_at
        + block * shape["per"]
        + quotient(remainder(send_row, patch_rows), 4) * (patch_cols // 4)
        + quotient(remainder(send_col, patch_cols), 4)
    )
    return jnp.where(sender < 0, 0, jnp.where(is_near, near_index, far_index))


def gather_kernel(
    shape,
    patch_rows,
    patch_cols,
    tile_nodes,
    node_hbm,
    edge_hbm,
    send_hbm,
    recv_hbm,
    tile_hbm,
    w_hbm,
    w_second_hbm,
    edge_gain_hbm,
    w_node_first_hbm,
    w_node_second_hbm,
    node_gain_hbm,
    first_ref,
    sent_ref,
    index_ref,
    edge_ref,
    recv_ref,
    own_ref,
    node_first_ref,
    w_second_ref,
    edge_gain_ref,
    w_node_sum_ref,
    w_node_second_ref,
    node_gain_ref,
    send_ref,
    tile_ref,
    w_ref,
    w_node_own_ref,
    flat_ref,
    side_ref,
    table_ref,
    received_ref,
    load_sem,
    halo_send,
    halo_recv,
    line_send,
    line_recv,
    plane_send,
    plane_recv,
    core_send,
    core_recv,
):
    lat_count, lon_count = lax.axis_size("lat"), lax.axis_size("lon")
    lat, lon = lax.axis_index("lat"), lax.axis_index("lon")
    cores, wide, high_count, low_count = (shape[k] for k in ("cores", "wide", "high", "low"))
    per = shape["per"]
    node_count, features = own_ref.shape
    left, right, top, bottom, corners, coarse_at = (at - node_count for at in shape["near"])
    core, across = lax.rem(lat, cores), lax.div(lat, cores)
    high, low = lax.div(lon, low_count), lax.rem(lon, low_count)
    tiles = features // LANES
    blocks, block_len = recv_ref.shape

    def load(source, target, i):
        return pltpu.make_async_copy(source, target, load_sem.at[i])

    loads = [
        load(source, target, i)
        for i, (source, target) in enumerate(
            (
                (node_hbm, own_ref),
                (w_hbm, w_ref),
                (send_hbm, send_ref),
                (recv_hbm, recv_ref),
                (tile_hbm, tile_ref),
                (edge_hbm, edge_ref),
                (w_node_first_hbm.at[pl.ds(0, features), :], w_node_own_ref),
                (w_node_first_hbm.at[pl.ds(features, features), :], w_node_sum_ref),
                (w_second_hbm, w_second_ref),
                (w_node_second_hbm, w_node_second_ref),
                (edge_gain_hbm, edge_gain_ref),
                (node_gain_hbm, node_gain_ref),
            )
        )
    ]
    loads[0].start()

    def device(at_across, at_core, at_high, at_low):
        return at_across * cores + at_core, at_high * low_count + at_low

    offsets = [(a, b) for a in range(wide) for b in range(low_count)][1:]

    def turn(at, step, count):
        return lax.rem(at + step, count) if step else at

    def line_to(k):
        return device(across, core, turn(high, k, high_count), low)

    def plane_to(step):
        return device(turn(across, step[0], wide), core, high, turn(low, step[1], low_count))

    partner = device(across, 1 - core, high, low)

    last = patch_rows
    halos = (
        (side_ref, last, patch_rows, left, 0, 1),
        (side_ref, 0, patch_rows, right, 0, -1),
        (own_ref, node_count - patch_cols, patch_cols, top, 1, 0),
        (own_ref, 0, patch_cols, bottom, -1, 0),
        (side_ref, last + patch_rows - 8, 8, corners, 1, 1),
        (side_ref, last, 8, corners + 8, -1, 1),
        (side_ref, patch_rows - 8, 8, corners + 16, 1, -1),
        (side_ref, 0, 8, corners + 24, -1, -1),
    )

    def halo_to(i):
        return (
            lax.rem(lat + halos[i][4] + lat_count, lat_count),
            lax.rem(lon + halos[i][5] + lon_count, lon_count),
        )

    barrier = pltpu.get_barrier_semaphore()
    greeted = [line_to(k) for k in range(1, high_count)] + [plane_to(step) for step in offsets]
    greeted += [partner] if cores == 2 else []
    greeted += [halo_to(i) for i in range(len(halos))]
    for at in greeted:
        pl.semaphore_signal(
            barrier, inc=1, device_id=at, device_id_type=pl.DeviceIdType.MESH
        )
    def slots(at_high, at_core, at_across, at_low, count=1):
        block = ((at_high * cores + at_core) * wide + at_across) * low_count + at_low
        return pl.ds(pl.multiple_of(coarse_at + block * per, 8), count * per)

    def copy(source, target, send_sem, recv_sem, at):
        return pltpu.make_async_remote_copy(
            src_ref=source,
            dst_ref=target,
            send_sem=send_sem,
            recv_sem=recv_sem,
            device_id=at,
            device_id_type=pl.DeviceIdType.MESH,
        )

    def line(k, origin):
        block = table_ref.at[slots(origin, core, across, low), :]
        return copy(block, block, line_send.at[k], line_recv.at[k], line_to(k))

    def line_out(k):
        return line(k, high)

    def line_in(k):
        return line(k, turn(high, high_count - k, high_count))

    def from_high(j):
        return turn(high, (high_count - j) % high_count, high_count)

    def plane(j, i, at_across, at_low):
        block = table_ref.at[slots(from_high(j), core, at_across, at_low), :]
        return copy(block, block, plane_send.at[j, i], plane_recv.at[j, i], plane_to(offsets[i]))

    def plane_out(j, i):
        return plane(j, i, across, low)

    def plane_in(j, i):
        a, b = offsets[i]
        return plane(
            j,
            i,
            turn(across, (wide - a) % wide, wide),
            turn(low, (low_count - b) % low_count, low_count),
        )

    def pair(j, at_core):
        block = table_ref.at[slots(from_high(j), at_core, 0, 0, wide * low_count), :]
        return copy(block, block, core_send.at[j], core_recv.at[j], partner)

    def halo(i):
        ref, start, size, target, _, _ = halos[i]
        return copy(
            ref.at[start : start + size, :],
            table_ref.at[target : target + size, :],
            halo_send.at[i],
            halo_recv.at[i],
            halo_to(i),
        )

    def sends(i):
        there = lat + halos[i][4]
        return (there >= 0) & (there < lat_count)

    def receives(i):
        origin = lat - halos[i][4]
        return (origin >= 0) & (origin < lat_count)

    def flatten(rows):
        for t in range(tiles):
            flat_ref[pl.ds(t * node_count + rows.start, rows.stop - rows.start), :] = own_ref[
                rows, t * LANES : (t + 1) * LANES
            ].astype(F32)

    def picked(start, count, step):
        parts = [
            flat_ref[pl.ds(t * node_count + start, count, stride=step), :] for t in range(tiles)
        ]
        return jnp.concatenate(parts, axis=1).astype(BF16)

    loads[0].wait()
    coarse = []
    for r in range(0, patch_rows, 4):
        flatten(slice(r * patch_cols, (r + 1) * patch_cols))
        coarse.append(picked(r * patch_cols, patch_cols // 4, 4))
    table_ref[slots(high, core, across, low), :] = jnp.concatenate(coarse, axis=0)
    for each in loads[1:]:
        each.start()
    for r in range(0, patch_rows, 4):
        flatten(slice((r + 1) * patch_cols, (r + 4) * patch_cols))
    side_ref[:patch_rows, :] = picked(0, patch_rows, patch_cols)
    side_ref[patch_rows:, :] = picked(patch_cols - 1, patch_rows, patch_cols)
    for i, (_, _, size, target, _, _) in enumerate(halos):

        @pl.when(jnp.logical_not(receives(i)))
        def _():
            table_ref[target : target + size, :] = jnp.zeros((size, features), BF16)

    pl.semaphore_wait(barrier, len(greeted))
    for k in range(1, high_count):
        line_out(k).start()
    for i in range(len(offsets)):
        plane_out(0, i).start()
    for i in range(len(halos)):
        pl.when(sends(i))(lambda i=i: halo(i).start())

    def relay_line(k):
        line_in(k).wait_recv()
        for i in range(len(offsets)):
            plane_out(k, i).start()

    def relay_plane(j):
        for i in range(len(offsets)):
            plane_in(j, i).wait_recv()
        if cores == 2:
            pair(j, core).start()

    def project(rows, start):
        result = 0.5 * dot(rows, w_ref[features : 2 * features, :])
        for t in range(tiles):
            sent_ref[pl.ds(start * tiles + t, rows.shape[0], stride=tiles), :] = result[
                :, t * LANES : (t + 1) * LANES
            ]

    def project_coarse(j):
        if cores == 2:
            pair(j, 1 - core).wait_recv()
        count = cores * wide * low_count * per
        rows = slots(from_high(j), 0, 0, 0, cores * wide * low_count)
        start = pl.multiple_of(node_count + coarse_at + from_high(j) * count, 8)
        project(table_ref[rows, :], start)

    def first_layer(g, size):
        rows = slice(g * size, (g + 1) * size)
        received = []
        for i in range(g * size // block_len, (g + 1) * size // block_len):
            local = recv_ref[i : i + 1, :] + tile_ref[i] * tile_nodes
            spread = jnp.broadcast_to(local, (LANES, block_len)).T
            lane = lax.broadcasted_iota(jnp.int32, (block_len, LANES), 1)
            parts = [
                jnp.where(spread == lane + at, 1.0, 0.0).astype(BF16)
                for at in range(0, node_count, LANES)
            ]
            received.append(jnp.concatenate(parts, axis=1))
        result = dot(edge_ref[rows, :], w_ref[:features, :]) + dot(
            jnp.concatenate(received, axis=0), received_ref[...]
        )
        first_ref[rows, :] = 0.5 * result

    loads[2].wait()
    index_ref[...] = tiles * sender_rows(
        send_ref[...], lat, lon, patch_rows, patch_cols, lon_count, shape
    )
    loads[1].wait()
    received_ref[...] = dot(own_ref[...], w_ref[2 * features :, :]).astype(BF16)
    project(own_ref[...], 0)
    loads[3].wait()
    loads[4].wait()
    loads[5].wait()

    groups = 8 if blocks % 8 == 0 else 1
    size = blocks * block_len // groups
    work = [functools.partial(first_layer, g, size) for g in range(groups)]

    def do(count):
        for _ in range(min(count, len(work))):
            work.pop(0)()

    for k in range(1, high_count):
        relay_line(k)
        do(1)
    relay_plane(0)
    do(2)
    for j in range(1, high_count):
        relay_plane(j)
        do(1)
        if j == 1:
            do(len(work))
            for i in range(len(halos)):
                pl.when(receives(i))(lambda i=i: halo(i).wait_recv())
            project(table_ref[:coarse_at, :], node_count)
        project_coarse(j - 1)
    do(len(work))
    project_coarse(high_count - 1)

    loads[6].wait()
    node_first_ref[...] = 0.5 * dot(own_ref[...], w_node_own_ref[...])
    for each in loads[7:]:
        each.wait()
    for k in range(1, high_count):
        line_out(k).wait_send()
    for j in range(high_count):
        for i in range(len(offsets)):
            plane_out(j, i).wait_send()
        if cores == 2:
            pair(j, core).wait_send()
    for i in range(len(halos)):
        pl.when(sends(i))(lambda i=i: halo(i).wait_send())


def in_hbm(*arrays):
    return [pltpu.with_memory_space_constraint(each, pltpu.HBM) for each in arrays]


def gather(shape, node, edges, senders, receivers, block_tile, weights, patch_rows, patch_cols):
    node_count, features = node.shape
    edge_count = edges.shape[0]
    blocks, block_len = receivers.shape
    tiles = features // LANES
    high = shape["high"]
    others = max(shape["wide"] * shape["low"] - 1, 1)
    dma = pltpu.SemaphoreType.DMA
    hbm, vmem = pl.BlockSpec(memory_space=pltpu.HBM), pl.BlockSpec(memory_space=pltpu.VMEM)
    out_shape = [
        pltpu.VMEM((edge_count, features), F32),
        pltpu.VMEM((shape["length"] * tiles, LANES), F32),
        pltpu.VMEM((blocks, block_len), jnp.int32),
        pltpu.VMEM((edge_count, features), BF16),
        pltpu.VMEM((blocks, block_len), jnp.int32),
        pltpu.VMEM((node_count, features), BF16),
        pltpu.VMEM((node_count, features), F32),
        pltpu.VMEM((features, features), BF16),
        pltpu.VMEM((1, features), F32),
        pltpu.VMEM((features, features), BF16),
        pltpu.VMEM((features, features), BF16),
        pltpu.VMEM((1, features), F32),
    ]
    operands = (node, edges, senders, receivers, block_tile, *weights)
    return pl.pallas_call(
        functools.partial(gather_kernel, shape, patch_rows, patch_cols, 4 * patch_cols),
        in_specs=[hbm] * len(operands),
        out_specs=[vmem] * len(out_shape),
        out_shape=out_shape,
        scratch_shapes=[
            pltpu.VMEM((blocks, block_len), jnp.int32),
            pltpu.SMEM((blocks,), jnp.int32),
            pltpu.VMEM(weights[0].shape, BF16),
            pltpu.VMEM((features, features), BF16),
            pltpu.VMEM((node_count * tiles, LANES), F32),
            pltpu.VMEM((2 * patch_rows, features), BF16),
            pltpu.VMEM((shape["length"] - node_count, features), BF16),
            pltpu.VMEM((node_count, features), BF16),
            dma((12,)),
            dma((8,)),
            dma((8,)),
            dma((high,)),
            dma((high,)),
            dma((high, others)),
            dma((high, others)),
            dma((high,)),
            dma((high,)),
        ],
        compiler_params=pltpu.CompilerParams(
            has_side_effects=True, collective_id=0, vmem_limit_bytes=16 * MIB
        ),
        cost_estimate=pl.CostEstimate(
            flops=8 * edge_count * features * features, bytes_accessed=8 * MIB, transcendentals=0
        ),
    )(*in_hbm(*operands))


def update_kernel(
    group,
    tile_nodes,
    tile_hbm,
    index_ref,
    first_ref,
    sent_ref,
    edge_ref,
    recv_ref,
    own_ref,
    node_first_ref,
    w_second_ref,
    edge_gain_ref,
    w_node_sum_ref,
    w_node_second_ref,
    node_gain_ref,
    node_out_hbm,
    edge_out_hbm,
    tile_ref,
    picked_ref,
    hidden_ref,
    second_ref,
    message_ref,
    edge_out_ref,
    total_ref,
    node_out_ref,
    load_sem,
    out_sem,
):
    edge_count, features = edge_ref.shape
    node_count = own_ref.shape[0]
    tiles = features // LANES
    block_len = recv_ref.shape[1]
    groups = edge_count // group
    tile_load = pltpu.make_async_copy(tile_hbm, tile_ref, load_sem)
    tile_load.start()
    total_ref[...] = jnp.zeros_like(total_ref)

    def pick(g):
        slot = g % 2
        for e in range(group):
            at = g * group + e
            start = pl.multiple_of(index_ref[at // block_len, at % block_len], tiles)
            picked_ref[slot, e * tiles : (e + 1) * tiles, :] = sent_ref[pl.ds(start, tiles), :]

    def hide(g):
        slot = g % 2
        for r in range(0, group, CHUNK):
            at = g * group + r
            parts = []
            for t in range(tiles):
                half = (
                    first_ref[at : at + CHUNK, t * LANES : (t + 1) * LANES]
                    + picked_ref[slot, pl.ds(r * tiles + t, CHUNK, stride=tiles), :]
                )
                parts.append((half + half * jnp.tanh(half)).astype(BF16))
            hidden_ref[slot, r : r + CHUNK, :] = jnp.concatenate(parts, axis=1)

    def finish(g):
        slot = g % 2
        for i in range(group // block_len):
            block = g * (group // block_len) + i
            receiver = recv_ref[block : block + 1, :]
            spread = jnp.broadcast_to(receiver, (LANES, block_len)).T
            live = jnp.where(spread >= 0, 1.0, 0.0).astype(BF16)
            for r in range(i * block_len, (i + 1) * block_len, CHUNK):
                at = g * group + r
                second = second_ref[slot, r : r + CHUNK, :]
                message = layer_norm(second, edge_gain_ref[...]).astype(BF16)
                message_ref[slot, r : r + CHUNK, :] = message
                mask = live[r % block_len : r % block_len + CHUNK, :]
                mask = jnp.concatenate([mask] * tiles, axis=1)
                edge_out_ref[at : at + CHUNK, :] = (edge_ref[at : at + CHUNK, :] + message) * mask
            start = pl.multiple_of(tile_ref[block] * tile_nodes, tile_nodes)
            node = lax.broadcasted_iota(jnp.int32, (tile_nodes, block_len), 0)
            hot = jnp.where(node == receiver, 1.0, 0.0).astype(BF16)
            total_ref[pl.ds(start, tile_nodes), :] += dot(
                hot, message_ref[slot, i * block_len : (i + 1) * block_len, :]
            )

    def store(g):
        rows = pl.ds(g * group, group)
        return pltpu.make_async_copy(
            edge_out_ref.at[rows, :], edge_out_hbm.at[rows, :], out_sem.at[g]
        )

    for g in range(groups):
        pick(g)
        hide(g)
        second_ref[g % 2] = dot(hidden_ref[g % 2], w_second_ref[...])
        if g == 0:
            tile_load.wait()
        finish(g)
        store(g).start()

    for at in range(0, node_count, tile_nodes):
        rows = slice(at, at + tile_nodes)
        half = node_first_ref[rows, :] + 0.5 * dot(
            total_ref[rows, :].astype(BF16), w_node_sum_ref[...]
        )
        node_hidden = (half + half * jnp.tanh(half)).astype(BF16)
        node_second = dot(node_hidden, w_node_second_ref[...])
        node_out_ref[rows, :] = (
            own_ref[rows, :].astype(F32) + layer_norm(node_second, node_gain_ref[...])
        ).astype(BF16)
    node_store = pltpu.make_async_copy(node_out_ref, node_out_hbm, out_sem.at[groups])
    node_store.start()
    for g in range(groups):
        store(g).wait()
    node_store.wait()


def update(block_tile, gathered, tile_nodes):
    edge_count, features = gathered[0].shape
    node_count = gathered[5].shape[0]
    blocks, block_len = gathered[4].shape
    tiles = features // LANES
    group = 4 * block_len if blocks % 4 == 0 else block_len
    groups = edge_count // group
    hbm, vmem = pl.BlockSpec(memory_space=pltpu.HBM), pl.BlockSpec(memory_space=pltpu.VMEM)
    first, sent, index, *rest = gathered
    return pl.pallas_call(
        functools.partial(update_kernel, group, tile_nodes),
        in_specs=[hbm, pl.BlockSpec(memory_space=pltpu.SMEM)] + [vmem] * (2 + len(rest)),
        out_specs=[hbm, hbm],
        out_shape=[
            jax.ShapeDtypeStruct((node_count, features), BF16),
            jax.ShapeDtypeStruct((edge_count, features), BF16),
        ],
        scratch_shapes=[
            pltpu.SMEM((blocks,), jnp.int32),
            pltpu.VMEM((2, group * tiles, LANES), F32),
            pltpu.VMEM((2, group, features), BF16),
            pltpu.VMEM((2, group, features), F32),
            pltpu.VMEM((2, group, features), BF16),
            pltpu.VMEM((edge_count, features), BF16),
            pltpu.VMEM((node_count, features), F32),
            pltpu.VMEM((node_count, features), BF16),
            pltpu.SemaphoreType.DMA,
            pltpu.SemaphoreType.DMA((groups + 1,)),
        ],
        compiler_params=pltpu.CompilerParams(vmem_limit_bytes=16 * MIB),
    )(*in_hbm(block_tile), index, first, sent, *rest)


def per_device(
    node_latent,
    edge_latent,
    sender,
    receiver,
    block_tile,
    w_first,
    w_second,
    edge_gain,
    w_node_first,
    w_node_second,
    node_gain,
):
    patch_rows, patch_cols, features = node_latent.shape
    blocks = block_tile.shape[0]
    shape = plan(patch_rows, patch_cols, lax.axis_size("lat"), lax.axis_size("lon"))
    node = node_latent.reshape(patch_rows * patch_cols, features)
    weights = (
        w_first,
        w_second,
        edge_gain.reshape(1, -1),
        w_node_first,
        w_node_second,
        node_gain.reshape(1, -1),
    )
    gathered = gather(
        shape,
        node,
        edge_latent,
        sender.reshape(blocks, -1),
        receiver.reshape(blocks, -1),
        block_tile,
        weights,
        patch_rows,
        patch_cols,
    )
    node_out, edge_out = update(block_tile, gathered, 4 * patch_cols)
    return node_out.reshape(patch_rows, patch_cols, features), edge_out


def solution(mesh):
    return jax.shard_map(
        per_device,
        mesh=mesh,
        in_specs=(
            P("lat", "lon", None),
            P(("lat", "lon"), None),
            P(("lat", "lon")),
            P(("lat", "lon")),
            P(("lat", "lon")),
            P(),
            P(),
            P(),
            P(),
            P(),
            P(),
        ),
        out_specs=(P("lat", "lon", None), P(("lat", "lon"), None)),
        check_vma=False,
    )
```

```python
import functools

import jax
import jax.numpy as jnp
from jax import lax
from jax.experimental import pallas as pl
from jax.experimental.pallas import tpu as pltpu
from jax.sharding import PartitionSpec as P

F32 = jnp.float32
BF16 = jnp.bfloat16
LANES = 128
CHUNK = 32
MIB = 1024 * 1024


def dot(a, b):
    return jnp.dot(a, b, preferred_element_type=F32)


def layer_norm(values, gain_vec):
    average = jnp.mean(values, -1, keepdims=True)
    centred = values - average
    spread = jnp.mean(centred * centred, -1, keepdims=True)
    return centred * lax.rsqrt(spread + 1e-05) * gain_vec


def power_of_two(n):
    return n & (n - 1) == 0


def quotient(value, n):
    if power_of_two(n):
        return lax.shift_right_arithmetic(value, jnp.full_like(value, n.bit_length() - 1))
    return lax.div(value, jnp.full_like(value, n))


def remainder(value, n):
    if power_of_two(n):
        return value & (n - 1)
    return lax.rem(value, jnp.full_like(value, n))


def plan(patch_rows, patch_cols, lat_count, lon_count):
    cores = 2 if lat_count % 2 == 0 else 1
    low = 1
    while lon_count % (4 * low) == 0 and 4 * low * low <= lon_count:
        low *= 2
    left = patch_rows * patch_cols
    right = left + patch_rows
    top = right + patch_rows
    bottom = top + patch_cols
    corners = bottom + patch_cols
    coarse_at = corners + 32
    per = patch_rows // 4 * (patch_cols // 4)
    return dict(
        cores=cores,
        wide=lat_count // cores,
        high=lon_count // low,
        low=low,
        near=(left, right, top, bottom, corners, coarse_at),
        per=per,
        length=coarse_at + per * lat_count * lon_count,
    )


def sender_rows(sender, lat, lon, patch_rows, patch_cols, lon_count, shape):
    grid_cols = patch_cols * lon_count
    left, right, top, bottom, corners, coarse_at = shape["near"]
    send_row, send_col = quotient(sender, grid_cols), remainder(sender, grid_cols)
    row = send_row - lat * patch_rows
    col = remainder(send_col - lon * patch_cols + 1 + grid_cols, grid_cols) - 1
    is_near = (row >= -1) & (row <= patch_rows) & (col <= patch_cols)
    inside = (col >= 0) & (col < patch_cols)
    side = jnp.where(col < 0, left, right)
    corner = corners + jnp.where(col < 0, 0, 16)
    top_index = jnp.where(inside, top + col, corner + 7)
    bottom_index = jnp.where(inside, bottom + col, corner + 8)
    middle = jnp.where(inside, row * patch_cols + col, side + row)
    near_index = jnp.where(row < 0, top_index, jnp.where(row >= patch_rows, bottom_index, middle))
    at_lat, at_lon = quotient(send_row, patch_rows), quotient(send_col, patch_cols)
    core, across = remainder(at_lat, shape["cores"]), quotient(at_lat, shape["cores"])
    high, low = quotient(at_lon, shape["low"]), remainder(at_lon, shape["low"])
    block = ((high * shape["cores"] + core) * shape["wide"] + across) * shape["low"] + low
    far_index = (
        coarse_at
        + block * shape["per"]
        + quotient(remainder(send_row, patch_rows), 4) * (patch_cols // 4)
        + quotient(remainder(send_col, patch_cols), 4)
    )
    return jnp.where(sender < 0, 0, jnp.where(is_near, near_index, far_index))


def gather_kernel(
    shape,
    patch_rows,
    patch_cols,
    tile_nodes,
    node_hbm,
    edge_hbm,
    send_hbm,
    recv_hbm,
    tile_hbm,
    w_hbm,
    w_second_hbm,
    edge_gain_hbm,
    w_node_first_hbm,
    w_node_second_hbm,
    node_gain_hbm,
    first_ref,
    sent_ref,
    index_ref,
    tile_ref,
    edge_ref,
    recv_ref,
    own_ref,
    node_first_ref,
    w_second_ref,
    edge_gain_ref,
    w_node_sum_ref,
    w_node_second_ref,
    node_gain_ref,
    send_ref,
    rows_ref,
    w_ref,
    w_node_own_ref,
    flat_ref,
    side_ref,
    table_ref,
    received_ref,
    index_sem,
    load_sem,
    halo_send,
    halo_recv,
    line_send,
    line_recv,
    plane_send,
    plane_recv,
    core_send,
    core_recv,
):
    lat_count, lon_count = lax.axis_size("lat"), lax.axis_size("lon")
    lat, lon = lax.axis_index("lat"), lax.axis_index("lon")
    cores, wide, high_count, low_count = (shape[k] for k in ("cores", "wide", "high", "low"))
    per = shape["per"]
    node_count, features = own_ref.shape
    left, right, top, bottom, corners, coarse_at = (at - node_count for at in shape["near"])
    core, across = lax.rem(lat, cores), lax.div(lat, cores)
    high, low = lax.div(lon, low_count), lax.rem(lon, low_count)
    tiles = features // LANES
    blocks, block_len = recv_ref.shape

    def load(source, target, i):
        return pltpu.make_async_copy(source, target, load_sem.at[i])

    loads = [
        load(source, target, i)
        for i, (source, target) in enumerate(
            (
                (node_hbm, own_ref),
                (w_hbm, w_ref),
                (send_hbm, send_ref),
                (recv_hbm, recv_ref),
                (tile_hbm, tile_ref),
                (edge_hbm, edge_ref),
                (w_node_first_hbm.at[pl.ds(0, features), :], w_node_own_ref),
                (w_node_first_hbm.at[pl.ds(features, features), :], w_node_sum_ref),
                (w_second_hbm, w_second_ref),
                (w_node_second_hbm, w_node_second_ref),
                (edge_gain_hbm, edge_gain_ref),
                (node_gain_hbm, node_gain_ref),
            )
        )
    ]
    for each in loads[:2]:
        each.start()

    def device(at_across, at_core, at_high, at_low):
        return at_across * cores + at_core, at_high * low_count + at_low

    offsets = [(a, b) for a in range(wide) for b in range(low_count)][1:]

    def turn(at, step, count):
        return lax.rem(at + step, count) if step else at

    def line_to(k):
        return device(across, core, turn(high, k, high_count), low)

    def plane_to(step):
        return device(turn(across, step[0], wide), core, high, turn(low, step[1], low_count))

    partner = device(across, 1 - core, high, low)

    last = patch_rows
    halos = (
        (side_ref, last, patch_rows, left, 0, 1),
        (side_ref, 0, patch_rows, right, 0, -1),
        (own_ref, node_count - patch_cols, patch_cols, top, 1, 0),
        (own_ref, 0, patch_cols, bottom, -1, 0),
        (side_ref, last + patch_rows - 8, 8, corners, 1, 1),
        (side_ref, last, 8, corners + 8, -1, 1),
        (side_ref, patch_rows - 8, 8, corners + 16, 1, -1),
        (side_ref, 0, 8, corners + 24, -1, -1),
    )

    def halo_to(i):
        return (
            lax.rem(lat + halos[i][4] + lat_count, lat_count),
            lax.rem(lon + halos[i][5] + lon_count, lon_count),
        )

    barrier = pltpu.get_barrier_semaphore()
    greeted = [line_to(k) for k in range(1, high_count)] + [plane_to(step) for step in offsets]
    greeted += [partner] if cores == 2 else []
    greeted += [halo_to(i) for i in range(len(halos))]
    for at in greeted:
        pl.semaphore_signal(
            barrier, inc=1, device_id=at, device_id_type=pl.DeviceIdType.MESH
        )
    def slots(at_high, at_core, at_across, at_low, count=1):
        block = ((at_high * cores + at_core) * wide + at_across) * low_count + at_low
        return pl.ds(pl.multiple_of(coarse_at + block * per, 8), count * per)

    def copy(source, target, send_sem, recv_sem, at):
        return pltpu.make_async_remote_copy(
            src_ref=source,
            dst_ref=target,
            send_sem=send_sem,
            recv_sem=recv_sem,
            device_id=at,
            device_id_type=pl.DeviceIdType.MESH,
        )

    def line(k, origin):
        block = table_ref.at[slots(origin, core, across, low), :]
        return copy(block, block, line_send.at[k], line_recv.at[k], line_to(k))

    def line_out(k):
        return line(k, high)

    def line_in(k):
        return line(k, turn(high, high_count - k, high_count))

    def from_high(j):
        return turn(high, (high_count - j) % high_count, high_count)

    def plane(j, i, at_across, at_low):
        block = table_ref.at[slots(from_high(j), core, at_across, at_low), :]
        return copy(block, block, plane_send.at[j, i], plane_recv.at[j, i], plane_to(offsets[i]))

    def plane_out(j, i):
        return plane(j, i, across, low)

    def plane_in(j, i):
        a, b = offsets[i]
        return plane(
            j,
            i,
            turn(across, (wide - a) % wide, wide),
            turn(low, (low_count - b) % low_count, low_count),
        )

    def pair(j, at_core):
        block = table_ref.at[slots(from_high(j), at_core, 0, 0, wide * low_count), :]
        return copy(block, block, core_send.at[j], core_recv.at[j], partner)

    def halo(i):
        ref, start, size, target, _, _ = halos[i]
        return copy(
            ref.at[start : start + size, :],
            table_ref.at[target : target + size, :],
            halo_send.at[i],
            halo_recv.at[i],
            halo_to(i),
        )

    def sends(i):
        there = lat + halos[i][4]
        return (there >= 0) & (there < lat_count)

    def receives(i):
        origin = lat - halos[i][4]
        return (origin >= 0) & (origin < lat_count)

    def flatten(rows):
        for t in range(tiles):
            flat_ref[pl.ds(t * node_count + rows.start, rows.stop - rows.start), :] = own_ref[
                rows, t * LANES : (t + 1) * LANES
            ].astype(F32)

    def picked(start, count, step):
        parts = [
            flat_ref[pl.ds(t * node_count + start, count, stride=step), :] for t in range(tiles)
        ]
        return jnp.concatenate(parts, axis=1).astype(BF16)

    loads[0].wait()
    coarse = []
    for r in range(0, patch_rows, 4):
        flatten(slice(r * patch_cols, (r + 1) * patch_cols))
        coarse.append(picked(r * patch_cols, patch_cols // 4, 4))
    table_ref[slots(high, core, across, low), :] = jnp.concatenate(coarse, axis=0)
    for each in loads[2:]:
        each.start()
    for r in range(0, patch_rows, 4):
        flatten(slice((r + 1) * patch_cols, (r + 4) * patch_cols))
    side_ref[:patch_rows, :] = picked(0, patch_rows, patch_cols)
    side_ref[patch_rows:, :] = picked(patch_cols - 1, patch_rows, patch_cols)
    for i, (_, _, size, target, _, _) in enumerate(halos):

        @pl.when(jnp.logical_not(receives(i)))
        def _():
            table_ref[target : target + size, :] = jnp.zeros((size, features), BF16)

    pl.semaphore_wait(barrier, len(greeted))
    for h in range(high_count):

        @pl.when(high == h)
        def _():
            for at in sorted(range(high_count), key=lambda at: -abs(at - h)):
                if at != h:
                    line_out((at - h) % high_count).start()

    for i in reversed(range(len(offsets))):
        plane_out(0, i).start()
    for i in range(len(halos)):
        pl.when(sends(i))(lambda i=i: halo(i).start())

    def relay_line(k):
        line_in(k).wait_recv()
        for i in reversed(range(len(offsets))):
            plane_out(k, i).start()

    def relay_plane(j):
        for i in range(len(offsets)):
            plane_in(j, i).wait_recv()
        if cores == 2:
            pair(j, core).start()

    def project(rows, start):
        result = 0.5 * dot(rows, w_ref[features : 2 * features, :])
        for t in range(tiles):
            sent_ref[pl.ds(start * tiles + t, rows.shape[0], stride=tiles), :] = result[
                :, t * LANES : (t + 1) * LANES
            ]

    def project_coarse(j):
        if cores == 2:
            pair(j, 1 - core).wait_recv()
        count = cores * wide * low_count * per
        rows = slots(from_high(j), 0, 0, 0, cores * wide * low_count)
        start = pl.multiple_of(node_count + coarse_at + from_high(j) * count, 8)
        project(table_ref[rows, :], start)

    def first_layer(g, size):
        rows = slice(g * size, (g + 1) * size)
        received = []
        for i in range(g * size // block_len, (g + 1) * size // block_len):
            local = recv_ref[i : i + 1, :] + tile_ref[i] * tile_nodes
            spread = jnp.broadcast_to(local, (LANES, block_len)).T
            lane = lax.broadcasted_iota(jnp.int32, (block_len, LANES), 1)
            parts = [
                jnp.where(spread == lane + at, 1.0, 0.0).astype(BF16)
                for at in range(0, node_count, LANES)
            ]
            received.append(jnp.concatenate(parts, axis=1))
        result = dot(edge_ref[rows, :], w_ref[:features, :]) + dot(
            jnp.concatenate(received, axis=0), received_ref[...]
        )
        first_ref[rows, :] = 0.5 * result

    loads[2].wait()
    rows_ref[...] = tiles * sender_rows(
        send_ref[...], lat, lon, patch_rows, patch_cols, lon_count, shape
    )
    loads[1].wait()
    received_ref[...] = dot(own_ref[...], w_ref[2 * features :, :]).astype(BF16)
    project(own_ref[...], 0)
    loads[3].wait()
    loads[4].wait()
    loads[5].wait()

    groups = 8 if blocks % 8 == 0 else 1
    size = blocks * block_len // groups
    work = [functools.partial(first_layer, g, size) for g in range(groups)]

    def do(count):
        for _ in range(min(count, len(work))):
            work.pop(0)()

    do(2)
    for k in range(1, high_count):
        relay_line(k)
        do(1)
    relay_plane(0)
    index_copy = pltpu.make_async_copy(rows_ref, index_ref, index_sem)
    index_copy.start()
    do(len(work))
    loads[6].wait()
    node_first_ref[...] = 0.5 * dot(own_ref[...], w_node_own_ref[...])
    for i in range(len(halos)):
        pl.when(receives(i))(lambda i=i: halo(i).wait_recv())
    project(table_ref[:coarse_at, :], node_count)
    for j in range(1, high_count):
        relay_plane(j)
        project_coarse(j - 1)
    project_coarse(high_count - 1)
    for each in loads[7:]:
        each.wait()
    index_copy.wait()
    for k in range(1, high_count):
        line_out(k).wait_send()
    for j in range(high_count):
        for i in range(len(offsets)):
            plane_out(j, i).wait_send()
        if cores == 2:
            pair(j, core).wait_send()
    for i in range(len(halos)):
        pl.when(sends(i))(lambda i=i: halo(i).wait_send())


def in_hbm(*arrays):
    return [pltpu.with_memory_space_constraint(each, pltpu.HBM) for each in arrays]


def gather(shape, node, edges, senders, receivers, block_tile, weights, patch_rows, patch_cols):
    node_count, features = node.shape
    edge_count = edges.shape[0]
    blocks, block_len = receivers.shape
    tiles = features // LANES
    high = shape["high"]
    others = max(shape["wide"] * shape["low"] - 1, 1)
    dma = pltpu.SemaphoreType.DMA
    hbm, vmem = pl.BlockSpec(memory_space=pltpu.HBM), pl.BlockSpec(memory_space=pltpu.VMEM)
    smem = pl.BlockSpec(memory_space=pltpu.SMEM)
    out_shape = [
        pltpu.VMEM((edge_count, features), F32),
        pltpu.VMEM((shape["length"] * tiles, LANES), F32),
        pltpu.SMEM((blocks, block_len), jnp.int32),
        pltpu.SMEM((blocks,), jnp.int32),
        pltpu.VMEM((edge_count, features), BF16),
        pltpu.VMEM((blocks, block_len), jnp.int32),
        pltpu.VMEM((node_count, features), BF16),
        pltpu.VMEM((node_count, features), F32),
        pltpu.VMEM((features, features), BF16),
        pltpu.VMEM((1, features), F32),
        pltpu.VMEM((features, features), BF16),
        pltpu.VMEM((features, features), BF16),
        pltpu.VMEM((1, features), F32),
    ]
    operands = (node, edges, senders, receivers, block_tile, *weights)
    return pl.pallas_call(
        functools.partial(gather_kernel, shape, patch_rows, patch_cols, 4 * patch_cols),
        in_specs=[hbm] * len(operands),
        out_specs=[vmem] * 2 + [smem] * 2 + [vmem] * 9,
        out_shape=out_shape,
        scratch_shapes=[
            pltpu.VMEM((blocks, block_len), jnp.int32),
            pltpu.VMEM((blocks, block_len), jnp.int32),
            pltpu.VMEM(weights[0].shape, BF16),
            pltpu.VMEM((features, features), BF16),
            pltpu.VMEM((node_count * tiles, LANES), F32),
            pltpu.VMEM((2 * patch_rows, features), BF16),
            pltpu.VMEM((shape["length"] - node_count, features), BF16),
            pltpu.VMEM((node_count, features), BF16),
            dma,
            dma((12,)),
            dma((8,)),
            dma((8,)),
            dma((high,)),
            dma((high,)),
            dma((high, others)),
            dma((high, others)),
            dma((high,)),
            dma((high,)),
        ],
        compiler_params=pltpu.CompilerParams(
            has_side_effects=True, collective_id=0, vmem_limit_bytes=16 * MIB
        ),
        cost_estimate=pl.CostEstimate(
            flops=8 * edge_count * features * features, bytes_accessed=8 * MIB, transcendentals=0
        ),
    )(*in_hbm(*operands))


def update_kernel(
    group,
    tile_nodes,
    first_ref,
    sent_ref,
    index_ref,
    tile_ref,
    edge_ref,
    recv_ref,
    own_ref,
    node_first_ref,
    w_second_ref,
    edge_gain_ref,
    w_node_sum_ref,
    w_node_second_ref,
    node_gain_ref,
    node_out_hbm,
    edge_out_hbm,
    picked_ref,
    hidden_ref,
    second_ref,
    message_ref,
    edge_out_ref,
    total_ref,
    node_out_ref,
    out_sem,
):
    edge_count, features = edge_ref.shape
    node_count = own_ref.shape[0]
    tiles = features // LANES
    block_len = recv_ref.shape[1]
    groups = edge_count // group
    total_ref[...] = jnp.zeros_like(total_ref)

    def pick(g):
        slot = g % 2
        for e in range(group):
            at = g * group + e
            start = pl.multiple_of(index_ref[at // block_len, at % block_len], tiles)
            picked_ref[slot, e * tiles : (e + 1) * tiles, :] = sent_ref[pl.ds(start, tiles), :]

    def hide(g):
        slot = g % 2
        for r in range(0, group, CHUNK):
            at = g * group + r
            parts = []
            for t in range(tiles):
                half = (
                    first_ref[at : at + CHUNK, t * LANES : (t + 1) * LANES]
                    + picked_ref[slot, pl.ds(r * tiles + t, CHUNK, stride=tiles), :]
                )
                parts.append((half + half * jnp.tanh(half)).astype(BF16))
            hidden_ref[slot, r : r + CHUNK, :] = jnp.concatenate(parts, axis=1)

    def finish(g):
        slot = g % 2
        for i in range(group // block_len):
            block = g * (group // block_len) + i
            receiver = recv_ref[block : block + 1, :]
            spread = jnp.broadcast_to(receiver, (LANES, block_len)).T
            live = jnp.where(spread >= 0, 1.0, 0.0).astype(BF16)
            for r in range(i * block_len, (i + 1) * block_len, CHUNK):
                at = g * group + r
                second = second_ref[slot, r : r + CHUNK, :]
                message = layer_norm(second, edge_gain_ref[...]).astype(BF16)
                message_ref[slot, r : r + CHUNK, :] = message
                mask = live[r % block_len : r % block_len + CHUNK, :]
                mask = jnp.concatenate([mask] * tiles, axis=1)
                edge_out_ref[at : at + CHUNK, :] = (edge_ref[at : at + CHUNK, :] + message) * mask
            start = pl.multiple_of(tile_ref[block] * tile_nodes, tile_nodes)
            node = lax.broadcasted_iota(jnp.int32, (tile_nodes, block_len), 0)
            hot = jnp.where(node == receiver, 1.0, 0.0).astype(BF16)
            total_ref[pl.ds(start, tile_nodes), :] += dot(
                hot, message_ref[slot, i * block_len : (i + 1) * block_len, :]
            )

    def store(g):
        rows = pl.ds(g * group, group)
        return pltpu.make_async_copy(
            edge_out_ref.at[rows, :], edge_out_hbm.at[rows, :], out_sem.at[g]
        )

    def node_store(at):
        rows = pl.ds(at, tile_nodes)
        return pltpu.make_async_copy(
            node_out_ref.at[rows, :],
            node_out_hbm.at[rows, :],
            out_sem.at[groups + at // tile_nodes],
        )

    for g in range(groups):
        pick(g)
        hide(g)
        second_ref[g % 2] = dot(hidden_ref[g % 2], w_second_ref[...])
        finish(g)
        store(g).start()

    for at in range(0, node_count, tile_nodes):
        rows = slice(at, at + tile_nodes)
        half = node_first_ref[rows, :] + 0.5 * dot(
            total_ref[rows, :].astype(BF16), w_node_sum_ref[...]
        )
        node_hidden = (half + half * jnp.tanh(half)).astype(BF16)
        node_second = dot(node_hidden, w_node_second_ref[...])
        node_out_ref[rows, :] = (
            own_ref[rows, :].astype(F32) + layer_norm(node_second, node_gain_ref[...])
        ).astype(BF16)
        node_store(at).start()
    for g in range(groups):
        store(g).wait()
    for at in range(0, node_count, tile_nodes):
        node_store(at).wait()


def update(gathered, tile_nodes):
    edge_count, features = gathered[0].shape
    blocks, block_len = gathered[2].shape
    node_count = gathered[6].shape[0]
    tiles = features // LANES
    group = 4 * block_len if blocks % 4 == 0 else block_len
    groups = edge_count // group
    hbm, vmem = pl.BlockSpec(memory_space=pltpu.HBM), pl.BlockSpec(memory_space=pltpu.VMEM)
    smem = pl.BlockSpec(memory_space=pltpu.SMEM)
    return pl.pallas_call(
        functools.partial(update_kernel, group, tile_nodes),
        in_specs=[vmem] * 2 + [smem] * 2 + [vmem] * (len(gathered) - 4),
        out_specs=[hbm, hbm],
        out_shape=[
            jax.ShapeDtypeStruct((node_count, features), BF16),
            jax.ShapeDtypeStruct((edge_count, features), BF16),
        ],
        scratch_shapes=[
            pltpu.VMEM((2, group * tiles, LANES), F32),
            pltpu.VMEM((2, group, features), BF16),
            pltpu.VMEM((2, group, features), F32),
            pltpu.VMEM((2, group, features), BF16),
            pltpu.VMEM((edge_count, features), BF16),
            pltpu.VMEM((node_count, features), F32),
            pltpu.VMEM((node_count, features), BF16),
            pltpu.SemaphoreType.DMA((groups + node_count // tile_nodes,)),
        ],
        compiler_params=pltpu.CompilerParams(vmem_limit_bytes=16 * MIB),
    )(*gathered)


def per_device(
    node_latent,
    edge_latent,
    sender,
    receiver,
    block_tile,
    w_first,
    w_second,
    edge_gain,
    w_node_first,
    w_node_second,
    node_gain,
):
    patch_rows, patch_cols, features = node_latent.shape
    blocks = block_tile.shape[0]
    shape = plan(patch_rows, patch_cols, lax.axis_size("lat"), lax.axis_size("lon"))
    node = node_latent.reshape(patch_rows * patch_cols, features)
    weights = (
        w_first,
        w_second,
        edge_gain.reshape(1, -1),
        w_node_first,
        w_node_second,
        node_gain.reshape(1, -1),
    )
    gathered = gather(
        shape,
        node,
        edge_latent,
        sender.reshape(blocks, -1),
        receiver.reshape(blocks, -1),
        block_tile,
        weights,
        patch_rows,
        patch_cols,
    )
    node_out, edge_out = update(gathered, 4 * patch_cols)
    return node_out.reshape(patch_rows, patch_cols, features), edge_out


def solution(mesh):
    return jax.shard_map(
        per_device,
        mesh=mesh,
        in_specs=(
            P("lat", "lon", None),
            P(("lat", "lon"), None),
            P(("lat", "lon")),
            P(("lat", "lon")),
            P(("lat", "lon")),
            P(),
            P(),
            P(),
            P(),
            P(),
            P(),
        ),
        out_specs=(P("lat", "lon", None), P(("lat", "lon"), None)),
        check_vma=False,
    )
```

```python
import functools

import jax
import jax.numpy as jnp
from jax import lax
from jax.experimental import pallas as pl
from jax.experimental.pallas import tpu as pltpu
from jax.sharding import PartitionSpec as P

F32 = jnp.float32
BF16 = jnp.bfloat16
LANES = 128
CHUNK = 32
MIB = 1024 * 1024


def dot(a, b):
    return jnp.dot(a, b, preferred_element_type=F32)


def layer_norm(values, gain_vec):
    average = jnp.mean(values, -1, keepdims=True)
    centred = values - average
    spread = jnp.mean(centred * centred, -1, keepdims=True)
    return centred * lax.rsqrt(spread + 1e-05) * gain_vec


def power_of_two(n):
    return n & (n - 1) == 0


def quotient(value, n):
    if power_of_two(n):
        return lax.shift_right_arithmetic(value, jnp.full_like(value, n.bit_length() - 1))
    return lax.div(value, jnp.full_like(value, n))


def remainder(value, n):
    if power_of_two(n):
        return value & (n - 1)
    return lax.rem(value, jnp.full_like(value, n))


def plan(patch_rows, patch_cols, lat_count, lon_count):
    cores = 2 if lat_count % 2 == 0 else 1
    low = 1
    while lon_count % (4 * low) == 0 and 4 * low * low <= lon_count:
        low *= 2
    left = patch_rows * patch_cols
    right = left + patch_rows
    top = right + patch_rows
    bottom = top + patch_cols
    corners = bottom + patch_cols
    coarse_at = corners + 32
    per = patch_rows // 4 * (patch_cols // 4)
    return dict(
        cores=cores,
        wide=lat_count // cores,
        high=lon_count // low,
        low=low,
        near=(left, right, top, bottom, corners, coarse_at),
        per=per,
        length=coarse_at + per * lat_count * lon_count,
    )


def sender_rows(sender, lat, lon, patch_rows, patch_cols, lon_count, shape):
    grid_cols = patch_cols * lon_count
    left, right, top, bottom, corners, coarse_at = shape["near"]
    send_row, send_col = quotient(sender, grid_cols), remainder(sender, grid_cols)
    row = send_row - lat * patch_rows
    col = remainder(send_col - lon * patch_cols + 1 + grid_cols, grid_cols) - 1
    is_near = (row >= -1) & (row <= patch_rows) & (col <= patch_cols)
    inside = (col >= 0) & (col < patch_cols)
    side = jnp.where(col < 0, left, right)
    corner = corners + jnp.where(col < 0, 0, 16)
    top_index = jnp.where(inside, top + col, corner + 7)
    bottom_index = jnp.where(inside, bottom + col, corner + 8)
    middle = jnp.where(inside, row * patch_cols + col, side + row)
    near_index = jnp.where(row < 0, top_index, jnp.where(row >= patch_rows, bottom_index, middle))
    at_lat, at_lon = quotient(send_row, patch_rows), quotient(send_col, patch_cols)
    core, across = remainder(at_lat, shape["cores"]), quotient(at_lat, shape["cores"])
    high, low = quotient(at_lon, shape["low"]), remainder(at_lon, shape["low"])
    block = ((high * shape["cores"] + core) * shape["wide"] + across) * shape["low"] + low
    far_index = (
        coarse_at
        + block * shape["per"]
        + quotient(remainder(send_row, patch_rows), 4) * (patch_cols // 4)
        + quotient(remainder(send_col, patch_cols), 4)
    )
    return jnp.where(sender < 0, 0, jnp.where(is_near, near_index, far_index))


def gather_kernel(
    shape,
    patch_rows,
    patch_cols,
    tile_nodes,
    node_hbm,
    edge_hbm,
    send_hbm,
    recv_hbm,
    tile_hbm,
    w_hbm,
    w_second_hbm,
    edge_gain_hbm,
    w_node_first_hbm,
    w_node_second_hbm,
    node_gain_hbm,
    first_ref,
    sent_ref,
    index_ref,
    tile_ref,
    edge_ref,
    recv_ref,
    own_ref,
    node_first_ref,
    w_second_ref,
    edge_gain_ref,
    w_node_sum_ref,
    w_node_second_ref,
    node_gain_ref,
    send_ref,
    rows_ref,
    w_ref,
    w_node_own_ref,
    flat_ref,
    side_ref,
    table_ref,
    received_ref,
    index_sem,
    load_sem,
    halo_send,
    halo_recv,
    line_send,
    line_recv,
    plane_send,
    plane_recv,
    core_send,
    core_recv,
):
    lat_count, lon_count = lax.axis_size("lat"), lax.axis_size("lon")
    lat, lon = lax.axis_index("lat"), lax.axis_index("lon")
    cores, wide, high_count, low_count = (shape[k] for k in ("cores", "wide", "high", "low"))
    per = shape["per"]
    node_count, features = own_ref.shape
    left, right, top, bottom, corners, coarse_at = (at - node_count for at in shape["near"])
    core, across = lax.rem(lat, cores), lax.div(lat, cores)
    high, low = lax.div(lon, low_count), lax.rem(lon, low_count)
    tiles = features // LANES
    blocks, block_len = recv_ref.shape

    def load(source, target, i):
        return pltpu.make_async_copy(source, target, load_sem.at[i])

    loads = [
        load(source, target, i)
        for i, (source, target) in enumerate(
            (
                (node_hbm, own_ref),
                (w_hbm, w_ref),
                (send_hbm, send_ref),
                (recv_hbm, recv_ref),
                (tile_hbm, tile_ref),
                (edge_hbm, edge_ref),
                (w_node_first_hbm.at[pl.ds(0, features), :], w_node_own_ref),
                (w_node_first_hbm.at[pl.ds(features, features), :], w_node_sum_ref),
                (w_second_hbm, w_second_ref),
                (w_node_second_hbm, w_node_second_ref),
                (edge_gain_hbm, edge_gain_ref),
                (node_gain_hbm, node_gain_ref),
            )
        )
    ]
    for each in loads[:2]:
        each.start()

    def device(at_across, at_core, at_high, at_low):
        return at_across * cores + at_core, at_high * low_count + at_low

    offsets = [(a, b) for a in range(wide) for b in range(low_count)][1:]

    def turn(at, step, count):
        return lax.rem(at + step, count) if step else at

    def line_to(k):
        return device(across, core, turn(high, k, high_count), low)

    def plane_to(step):
        return device(turn(across, step[0], wide), core, high, turn(low, step[1], low_count))

    partner = device(across, 1 - core, high, low)

    last = patch_rows
    halos = (
        (side_ref, last, patch_rows, left, 0, 1),
        (side_ref, 0, patch_rows, right, 0, -1),
        (own_ref, node_count - patch_cols, patch_cols, top, 1, 0),
        (own_ref, 0, patch_cols, bottom, -1, 0),
        (side_ref, last + patch_rows - 8, 8, corners, 1, 1),
        (side_ref, last, 8, corners + 8, -1, 1),
        (side_ref, patch_rows - 8, 8, corners + 16, 1, -1),
        (side_ref, 0, 8, corners + 24, -1, -1),
    )

    def halo_to(i):
        return (
            lax.rem(lat + halos[i][4] + lat_count, lat_count),
            lax.rem(lon + halos[i][5] + lon_count, lon_count),
        )

    barrier = pltpu.get_barrier_semaphore()
    greeted = [line_to(k) for k in range(1, high_count)] + [plane_to(step) for step in offsets]
    greeted += [partner] if cores == 2 else []
    greeted += [halo_to(i) for i in range(len(halos))]
    for at in greeted:
        pl.semaphore_signal(
            barrier, inc=1, device_id=at, device_id_type=pl.DeviceIdType.MESH
        )
    def slots(at_high, at_core, at_across, at_low, count=1):
        block = ((at_high * cores + at_core) * wide + at_across) * low_count + at_low
        return pl.ds(pl.multiple_of(coarse_at + block * per, 8), count * per)

    def copy(source, target, send_sem, recv_sem, at):
        return pltpu.make_async_remote_copy(
            src_ref=source,
            dst_ref=target,
            send_sem=send_sem,
            recv_sem=recv_sem,
            device_id=at,
            device_id_type=pl.DeviceIdType.MESH,
        )

    def line(k, origin):
        block = table_ref.at[slots(origin, core, across, low), :]
        return copy(block, block, line_send.at[k], line_recv.at[k], line_to(k))

    def line_out(k):
        return line(k, high)

    def line_in(k):
        return line(k, turn(high, high_count - k, high_count))

    def from_high(j):
        return turn(high, (high_count - j) % high_count, high_count)

    def plane(j, i, at_across, at_low):
        block = table_ref.at[slots(from_high(j), core, at_across, at_low), :]
        return copy(block, block, plane_send.at[j, i], plane_recv.at[j, i], plane_to(offsets[i]))

    def plane_out(j, i):
        return plane(j, i, across, low)

    def plane_in(j, i):
        a, b = offsets[i]
        return plane(
            j,
            i,
            turn(across, (wide - a) % wide, wide),
            turn(low, (low_count - b) % low_count, low_count),
        )

    def pair(j, at_core):
        block = table_ref.at[slots(from_high(j), at_core, 0, 0, wide * low_count), :]
        return copy(block, block, core_send.at[j], core_recv.at[j], partner)

    def halo(i):
        ref, start, size, target, _, _ = halos[i]
        return copy(
            ref.at[start : start + size, :],
            table_ref.at[target : target + size, :],
            halo_send.at[i],
            halo_recv.at[i],
            halo_to(i),
        )

    def sends(i):
        there = lat + halos[i][4]
        return (there >= 0) & (there < lat_count)

    def receives(i):
        origin = lat - halos[i][4]
        return (origin >= 0) & (origin < lat_count)

    def flatten(rows):
        for t in range(tiles):
            flat_ref[pl.ds(t * node_count + rows.start, rows.stop - rows.start), :] = own_ref[
                rows, t * LANES : (t + 1) * LANES
            ].astype(F32)

    def picked(start, count, step):
        parts = [
            flat_ref[pl.ds(t * node_count + start, count, stride=step), :] for t in range(tiles)
        ]
        return jnp.concatenate(parts, axis=1).astype(BF16)

    loads[0].wait()
    coarse = []
    for r in range(0, patch_rows, 4):
        flatten(slice(r * patch_cols, (r + 1) * patch_cols))
        coarse.append(picked(r * patch_cols, patch_cols // 4, 4))
    table_ref[slots(high, core, across, low), :] = jnp.concatenate(coarse, axis=0)
    for each in loads[2:]:
        each.start()
    for r in range(0, patch_rows, 4):
        flatten(slice((r + 1) * patch_cols, (r + 4) * patch_cols))
    side_ref[:patch_rows, :] = picked(0, patch_rows, patch_cols)
    side_ref[patch_rows:, :] = picked(patch_cols - 1, patch_rows, patch_cols)
    for i, (_, _, size, target, _, _) in enumerate(halos):

        @pl.when(jnp.logical_not(receives(i)))
        def _():
            table_ref[target : target + size, :] = jnp.zeros((size, features), BF16)

    pl.semaphore_wait(barrier, len(greeted))
    for h in range(high_count):

        @pl.when(high == h)
        def _():
            for at in sorted(range(high_count), key=lambda at: -abs(at - h)):
                if at != h:
                    line_out((at - h) % high_count).start()

    for i in reversed(range(len(offsets))):
        plane_out(0, i).start()
    for i in range(len(halos)):
        pl.when(sends(i))(lambda i=i: halo(i).start())

    def relay_line(k):
        line_in(k).wait_recv()
        for i in reversed(range(len(offsets))):
            plane_out(k, i).start()

    def relay_plane(j):
        for i in range(len(offsets)):
            plane_in(j, i).wait_recv()
        if cores == 2:
            pair(j, core).start()

    def project(rows, start):
        result = 0.5 * dot(rows, w_ref[features : 2 * features, :])
        for t in range(tiles):
            sent_ref[pl.ds(start * tiles + t, rows.shape[0], stride=tiles), :] = result[
                :, t * LANES : (t + 1) * LANES
            ]

    def project_coarse(j):
        if cores == 2:
            pair(j, 1 - core).wait_recv()
        count = cores * wide * low_count * per
        rows = slots(from_high(j), 0, 0, 0, cores * wide * low_count)
        start = pl.multiple_of(node_count + coarse_at + from_high(j) * count, 8)
        project(table_ref[rows, :], start)

    def first_layer(g, size):
        rows = slice(g * size, (g + 1) * size)
        received = []
        for i in range(g * size // block_len, (g + 1) * size // block_len):
            local = recv_ref[i : i + 1, :] + tile_ref[i] * tile_nodes
            spread = jnp.broadcast_to(local, (LANES, block_len)).T
            lane = lax.broadcasted_iota(jnp.int32, (block_len, LANES), 1)
            parts = [
                jnp.where(spread == lane + at, 1.0, 0.0).astype(BF16)
                for at in range(0, node_count, LANES)
            ]
            received.append(jnp.concatenate(parts, axis=1))
        result = dot(edge_ref[rows, :], w_ref[:features, :]) + dot(
            jnp.concatenate(received, axis=0), received_ref[...]
        )
        first_ref[rows, :] = 0.5 * result

    loads[2].wait()
    rows_ref[...] = tiles * sender_rows(
        send_ref[...], lat, lon, patch_rows, patch_cols, lon_count, shape
    )
    loads[1].wait()
    received_ref[...] = dot(own_ref[...], w_ref[2 * features :, :]).astype(BF16)
    project(own_ref[...], 0)
    loads[3].wait()
    loads[4].wait()
    loads[5].wait()

    groups = 8 if blocks % 8 == 0 else 1
    size = blocks * block_len // groups
    work = [functools.partial(first_layer, g, size) for g in range(groups)]

    def do(count):
        for _ in range(min(count, len(work))):
            work.pop(0)()

    do(2)
    for k in range(1, high_count):
        relay_line(k)
        do(1)
    relay_plane(0)
    index_copy = pltpu.make_async_copy(rows_ref, index_ref, index_sem)
    index_copy.start()
    do(len(work))
    loads[6].wait()
    node_first_ref[...] = 0.5 * dot(own_ref[...], w_node_own_ref[...])
    for i in range(len(halos)):
        pl.when(receives(i))(lambda i=i: halo(i).wait_recv())
    project(table_ref[:coarse_at, :], node_count)
    for j in range(1, high_count):
        relay_plane(j)
        project_coarse(j - 1)
    project_coarse(high_count - 1)
    for each in loads[7:]:
        each.wait()
    index_copy.wait()
    for k in range(1, high_count):
        line_out(k).wait_send()
    for j in range(high_count):
        for i in range(len(offsets)):
            plane_out(j, i).wait_send()
        if cores == 2:
            pair(j, core).wait_send()
    for i in range(len(halos)):
        pl.when(sends(i))(lambda i=i: halo(i).wait_send())


def in_hbm(*arrays):
    return [pltpu.with_memory_space_constraint(each, pltpu.HBM) for each in arrays]


def gather(shape, node, edges, senders, receivers, block_tile, weights, patch_rows, patch_cols):
    node_count, features = node.shape
    edge_count = edges.shape[0]
    blocks, block_len = receivers.shape
    tiles = features // LANES
    high = shape["high"]
    others = max(shape["wide"] * shape["low"] - 1, 1)
    dma = pltpu.SemaphoreType.DMA
    hbm, vmem = pl.BlockSpec(memory_space=pltpu.HBM), pl.BlockSpec(memory_space=pltpu.VMEM)
    smem = pl.BlockSpec(memory_space=pltpu.SMEM)
    out_shape = [
        pltpu.VMEM((edge_count, features), F32),
        pltpu.VMEM((shape["length"] * tiles, LANES), F32),
        pltpu.SMEM((blocks, block_len), jnp.int32),
        pltpu.SMEM((blocks,), jnp.int32),
        pltpu.VMEM((edge_count, features), BF16),
        pltpu.VMEM((blocks, block_len), jnp.int32),
        pltpu.VMEM((node_count, features), BF16),
        pltpu.VMEM((node_count, features), F32),
        pltpu.VMEM((features, features), BF16),
        pltpu.VMEM((1, features), F32),
        pltpu.VMEM((features, features), BF16),
        pltpu.VMEM((features, features), BF16),
        pltpu.VMEM((1, features), F32),
    ]
    operands = (node, edges, senders, receivers, block_tile, *weights)
    return pl.pallas_call(
        functools.partial(gather_kernel, shape, patch_rows, patch_cols, 4 * patch_cols),
        in_specs=[hbm] * len(operands),
        out_specs=[vmem] * 2 + [smem] * 2 + [vmem] * 9,
        out_shape=out_shape,
        scratch_shapes=[
            pltpu.VMEM((blocks, block_len), jnp.int32),
            pltpu.VMEM((blocks, block_len), jnp.int32),
            pltpu.VMEM(weights[0].shape, BF16),
            pltpu.VMEM((features, features), BF16),
            pltpu.VMEM((node_count * tiles, LANES), F32),
            pltpu.VMEM((2 * patch_rows, features), BF16),
            pltpu.VMEM((shape["length"] - node_count, features), BF16),
            pltpu.VMEM((node_count, features), BF16),
            dma,
            dma((12,)),
            dma((8,)),
            dma((8,)),
            dma((high,)),
            dma((high,)),
            dma((high, others)),
            dma((high, others)),
            dma((high,)),
            dma((high,)),
        ],
        compiler_params=pltpu.CompilerParams(
            has_side_effects=True, collective_id=0, vmem_limit_bytes=16 * MIB
        ),
        cost_estimate=pl.CostEstimate(
            flops=8 * edge_count * features * features, bytes_accessed=8 * MIB, transcendentals=0
        ),
    )(*in_hbm(*operands))


def update_kernel(
    group,
    tile_nodes,
    first_ref,
    sent_ref,
    index_ref,
    tile_ref,
    edge_ref,
    recv_ref,
    own_ref,
    node_first_ref,
    w_second_ref,
    edge_gain_ref,
    w_node_sum_ref,
    w_node_second_ref,
    node_gain_ref,
    node_out_hbm,
    edge_out_hbm,
    picked_ref,
    hidden_ref,
    second_ref,
    message_ref,
    edge_out_ref,
    total_ref,
    node_out_ref,
    out_sem,
):
    edge_count, features = edge_ref.shape
    node_count = own_ref.shape[0]
    tiles = features // LANES
    block_len = recv_ref.shape[1]
    groups = edge_count // group
    total_ref[...] = jnp.zeros_like(total_ref)

    def pick(g):
        slot = g % 2
        for e in range(group):
            at = g * group + e
            start = pl.multiple_of(index_ref[at // block_len, at % block_len], tiles)
            picked_ref[slot, e * tiles : (e + 1) * tiles, :] = sent_ref[pl.ds(start, tiles), :]

    def hide(g):
        slot = g % 2
        for r in range(0, group, CHUNK):
            at = g * group + r
            parts = []
            for t in range(tiles):
                half = (
                    first_ref[at : at + CHUNK, t * LANES : (t + 1) * LANES]
                    + picked_ref[slot, pl.ds(r * tiles + t, CHUNK, stride=tiles), :]
                )
                parts.append((half + half * jnp.tanh(half)).astype(BF16))
            hidden_ref[slot, r : r + CHUNK, :] = jnp.concatenate(parts, axis=1)

    def finish(g):
        slot = g % 2
        for i in range(group // block_len):
            block = g * (group // block_len) + i
            receiver = recv_ref[block : block + 1, :]
            spread = jnp.broadcast_to(receiver, (LANES, block_len)).T
            live = jnp.where(spread >= 0, 1.0, 0.0).astype(BF16)
            for r in range(i * block_len, (i + 1) * block_len, CHUNK):
                at = g * group + r
                second = second_ref[slot, r : r + CHUNK, :]
                message = layer_norm(second, edge_gain_ref[...]).astype(BF16)
                message_ref[slot, r : r + CHUNK, :] = message
                mask = live[r % block_len : r % block_len + CHUNK, :]
                mask = jnp.concatenate([mask] * tiles, axis=1)
                edge_out_ref[at : at + CHUNK, :] = (edge_ref[at : at + CHUNK, :] + message) * mask
            start = pl.multiple_of(tile_ref[block] * tile_nodes, tile_nodes)
            node = lax.broadcasted_iota(jnp.int32, (tile_nodes, block_len), 0)
            hot = jnp.where(node == receiver, 1.0, 0.0).astype(BF16)
            total_ref[pl.ds(start, tile_nodes), :] += dot(
                hot, message_ref[slot, i * block_len : (i + 1) * block_len, :]
            )

    def store(g):
        rows = pl.ds(g * group, group)
        return pltpu.make_async_copy(
            edge_out_ref.at[rows, :], edge_out_hbm.at[rows, :], out_sem.at[g]
        )

    def node_store(at):
        rows = pl.ds(at, tile_nodes)
        return pltpu.make_async_copy(
            node_out_ref.at[rows, :],
            node_out_hbm.at[rows, :],
            out_sem.at[groups + at // tile_nodes],
        )

    for g in range(groups):
        pick(g)
        hide(g)
        second_ref[g % 2] = dot(hidden_ref[g % 2], w_second_ref[...])
        finish(g)
        store(g).start()

    for at in range(0, node_count, tile_nodes):
        rows = slice(at, at + tile_nodes)
        half = node_first_ref[rows, :] + 0.5 * dot(
            total_ref[rows, :].astype(BF16), w_node_sum_ref[...]
        )
        node_hidden = (half + half * jnp.tanh(half)).astype(BF16)
        node_second = dot(node_hidden, w_node_second_ref[...])
        node_out_ref[rows, :] = (
            own_ref[rows, :].astype(F32) + layer_norm(node_second, node_gain_ref[...])
        ).astype(BF16)
        node_store(at).start()
    for g in range(groups):
        store(g).wait()
    for at in range(0, node_count, tile_nodes):
        node_store(at).wait()


def update(gathered, tile_nodes):
    edge_count, features = gathered[0].shape
    blocks, block_len = gathered[2].shape
    node_count = gathered[6].shape[0]
    tiles = features // LANES
    group = 8 * block_len if blocks % 8 == 0 else block_len
    groups = edge_count // group
    hbm, vmem = pl.BlockSpec(memory_space=pltpu.HBM), pl.BlockSpec(memory_space=pltpu.VMEM)
    smem = pl.BlockSpec(memory_space=pltpu.SMEM)
    return pl.pallas_call(
        functools.partial(update_kernel, group, tile_nodes),
        in_specs=[vmem] * 2 + [smem] * 2 + [vmem] * (len(gathered) - 4),
        out_specs=[hbm, hbm],
        out_shape=[
            jax.ShapeDtypeStruct((node_count, features), BF16),
            jax.ShapeDtypeStruct((edge_count, features), BF16),
        ],
        scratch_shapes=[
            pltpu.VMEM((2, group * tiles, LANES), F32),
            pltpu.VMEM((2, group, features), BF16),
            pltpu.VMEM((2, group, features), F32),
            pltpu.VMEM((2, group, features), BF16),
            pltpu.VMEM((edge_count, features), BF16),
            pltpu.VMEM((node_count, features), F32),
            pltpu.VMEM((node_count, features), BF16),
            pltpu.SemaphoreType.DMA((groups + node_count // tile_nodes,)),
        ],
        compiler_params=pltpu.CompilerParams(vmem_limit_bytes=28 * MIB),
    )(*gathered)


def per_device(
    node_latent,
    edge_latent,
    sender,
    receiver,
    block_tile,
    w_first,
    w_second,
    edge_gain,
    w_node_first,
    w_node_second,
    node_gain,
):
    patch_rows, patch_cols, features = node_latent.shape
    blocks = block_tile.shape[0]
    shape = plan(patch_rows, patch_cols, lax.axis_size("lat"), lax.axis_size("lon"))
    node = node_latent.reshape(patch_rows * patch_cols, features)
    weights = (
        w_first,
        w_second,
        edge_gain.reshape(1, -1),
        w_node_first,
        w_node_second,
        node_gain.reshape(1, -1),
    )
    gathered = gather(
        shape,
        node,
        edge_latent,
        sender.reshape(blocks, -1),
        receiver.reshape(blocks, -1),
        block_tile,
        weights,
        patch_rows,
        patch_cols,
    )
    node_out, edge_out = update(gathered, 4 * patch_cols)
    return node_out.reshape(patch_rows, patch_cols, features), edge_out


def solution(mesh):
    return jax.shard_map(
        per_device,
        mesh=mesh,
        in_specs=(
            P("lat", "lon", None),
            P(("lat", "lon"), None),
            P(("lat", "lon")),
            P(("lat", "lon")),
            P(("lat", "lon")),
            P(),
            P(),
            P(),
            P(),
            P(),
            P(),
        ),
        out_specs=(P("lat", "lon", None), P(("lat", "lon"), None)),
        check_vma=False,
    )
```
